256 devices in a mesh: batch: 8 (over x, z_hi), seq: 4 (over y), mp: 8 (over z_lo, core).
Axes of the slice: x: 4, y: 4, z: 8 (z_hi: 2, z_lo: 4; z = z_hi * 4 + z_lo), core: 2. Of those that a mesh axis runs over, the one named last changes fastest.
Arguments:
- context: bfloat16 [4096, 6144], P(('batch', 'seq'), 'mp'), may hold values from -0.1875 to 0.1875
- cotangent: bfloat16 [4096, 6144], P(('batch', 'seq'), 'mp'), may hold values from -6 to 6
- out_weight: bfloat16 [6144, 6144], P(None, 'mp'), may hold values from -0.078125 to 0.078125
Outputs:
- grad_weight: float32 [6144, 6144], P(('batch', 'seq'), 'mp')
- grad_context: bfloat16 [4096, 6144], P(('batch', 'seq'), 'mp')
The draws below stay inside these ranges and needn't reach their ends.
All inputs are finite; a program needn't handle non-finite values.
Results may differ from the reference program's by a relative error of at most 0.001.
Values may be sent and summed in bfloat16 or wider, within the bound.
No kernel may reach another device: no remote copies, remote signals or barrier semaphores. Data moves between devices by JAX's collectives and lax.ppermute only.
A program may use at most 64 MiB of HBM per device.

```python
import jax
import jax.numpy as jnp
from jax import lax

D = 6144
TOKENS = 4096


def strengthened(values, key, source, target, shards_of, factor):
    def block_of(dim):
        return (jnp.arange(values.shape[dim]) // (values.shape[dim] // shards_of)).reshape((-1,) + (1,) * (values.ndim - 1 - dim))

    near = jax.random.permutation(key, shards_of)[block_of(target)]
    other_side = (block_of(target) + shards_of // 2) % shards_of
    return jnp.where((block_of(source) == near) | (block_of(source) == other_side), factor * values, values)


def block_levels(stream_key, shape, pieces, least, largest):
    def one(dim, parts):
        heights = jax.random.uniform(jax.random.fold_in(jax.random.fold_in(stream_key, 6), dim), (parts,), jnp.float32, least / len(pieces), largest / len(pieces))
        return jnp.repeat(jnp.exp(heights), shape[dim] // parts).reshape((-1,) + (1,) * (len(shape) - dim - 1))

    gain = one(*pieces[0])
    for cut in pieces[1:]:
        gain = gain * one(*cut)
    return gain


def scatter_about(stream_key, dims, scale, limit, split=(), held_as=jnp.bfloat16):
    loudness = block_levels(stream_key, dims, split, -0.22, 0.18) if split else 1.0
    result = jax.random.normal(stream_key, dims, jnp.float32) * scale * loudness
    return jnp.minimum(jnp.maximum(result, -limit), limit).astype(held_as)


def gaussian_with(key, shape, scale, most, pieces, heavy, kind=jnp.bfloat16):
    entries = scale * jax.random.normal(key, shape, jnp.float32)
    if pieces:
        entries = entries * block_levels(key, shape, pieces, -0.22, 0.18)
    return jnp.clip(strengthened(entries, jax.random.fold_in(key, 3), *heavy), -most, most).astype(kind)


def setup_inputs(seed: int = 0) -> dict:
    splits = jax.random.split(jax.random.key(seed), 4)
    return {
        "context": gaussian_with(splits[0], (TOKENS, D), (1 / TOKENS ** 0.5), 0.1875, ((0, 32), (1, 8)), (0, 1, 32, 2.75)),
        "cotangent": scatter_about(splits[1], (TOKENS, D), 1.0, 6.0, ((0, 32), (1, 8))),
        "out_weight": scatter_about(splits[2], (D, D), D ** -0.5, 0.078125, ((1, 8),)),
    }


def reference(context, cotangent, out_weight):
    grad_weight = lax.dot_general(context, cotangent, (((0,), (0,)), ((), ())), preferred_element_type=jnp.float32)
    grad_context = lax.dot_general(cotangent, out_weight, (((1,), (1,)), ((), ())), preferred_element_type=jnp.float32)
    return grad_weight, grad_context.astype(jnp.bfloat16)
```

```python
import jax
import jax.numpy as jnp
from jax import lax
from jax.experimental import pallas as pl
from jax.experimental.pallas import tpu as pltpu
from jax.sharding import PartitionSpec as P


AXES = ("batch", "seq", "mp")
F32 = jnp.float32
BF16 = jnp.bfloat16


def pairs(route):
    out = []
    for x in range(4):
        for h in range(2):
            for y in range(4):
                for l in range(4):
                    for c in range(2):
                        a = place(x, h, y, l, c)
                        b = place(*route(x, h, y, l, c))
                        out.append((a, b))
    return out


def place(x, h, y, l, c):
    return ((x * 2 + h) * 4 + y) * 8 + l * 2 + c


def ring(step):
    def route(x, h, y, l, c):
        z = (4 * h + l + step) % 8
        return x, z // 4, y, z % 4, c

    return route


def send(array, route):
    return lax.ppermute(array, AXES, pairs(route))


def at(stack, index):
    return lax.dynamic_index_in_dim(stack, index, 0, keepdims=False)


def partial_kernel(index, left, weight, out):
    out[0] = lax.dot_general(
        left[0], weight[...], (((1,), (1,)), ((), ())), preferred_element_type=F32
    )


def partial_products(index, left, weight):
    n, rows, depth = left.shape
    width = depth
    return pl.pallas_call(
        partial_kernel,
        out_shape=jax.ShapeDtypeStruct((n, rows, width), F32),
        grid_spec=pltpu.PrefetchScalarGridSpec(
            num_scalar_prefetch=1,
            grid=(n,),
            in_specs=[
                pl.BlockSpec((1, rows, depth), lambda i, index: (i, 0, 0)),
                pl.BlockSpec((width, depth), lambda i, index: (index[i], 0)),
            ],
            out_specs=pl.BlockSpec((1, rows, width), lambda i, index: (i, 0, 0)),
        ),
        cost_estimate=pl.CostEstimate(
            flops=2 * n * rows * width * depth,
            bytes_accessed=n * width * depth * 2 + n * rows * width * 4,
            transcendentals=0,
        ),
    )(index, left, weight)


def weight_kernel(place_ref, own, other, *refs):
    cots, out = refs[:-1], refs[-1]
    low, mixed = place_ref[0], place_ref[1]
    total = jnp.zeros(out.shape, F32)
    for piece, cot in enumerate(cots):
        far = piece // 4
        for half in range(2):
            lefts = []
            for m in (2 * half, 2 * half + 1):
                r, s = (m, piece % 4) if far == 0 else (piece % 4, m)
                k = low ^ r
                mine, theirs = own[k, s], other[k, s]
                use_own = mixed == far
                lefts.append(jnp.where(use_own, mine, theirs))
            left = jnp.concatenate(lefts, axis=1)
            right = cot[pl.ds(256 * half, 256), :]
            total += jnp.dot(left, right, preferred_element_type=F32)
    out[...] = total


def weight_gradient(place_index, own, other, cots):
    rows, width = own.shape[2], cots[0].shape[1]
    vmem = pl.BlockSpec(memory_space=pltpu.VMEM)
    return pl.pallas_call(
        weight_kernel,
        out_shape=jax.ShapeDtypeStruct((rows, width), F32),
        in_specs=[pl.BlockSpec(memory_space=pltpu.SMEM)] + [vmem] * (2 + len(cots)),
        out_specs=vmem,
        cost_estimate=pl.CostEstimate(
            flops=2 * rows * width * 512 * len(cots),
            bytes_accessed=len(cots) * 512 * width * 2,
            transcendentals=0,
        ),
    )(place_index, own, other, *cots)


def shards(context, cotangent, out_weight):
    batch, y, mp = (lax.axis_index(a) for a in AXES)
    x, h = batch // 2, batch % 2
    l, c = mp // 2, mp % 2
    tokens, width = cotangent.shape
    quarter = width // 4

    def gather_x(a):
        return [a] + [
            send(a, lambda x, h, y, l, c, k=k: (x ^ k, h, y, l, c)) for k in (1, 2, 3)
        ]

    def gather_y(a):
        return [a] + [
            send(a, lambda x, h, y, l, c, k=k: (x, h, y ^ k, l, c)) for k in (1, 2, 3)
        ]

    far_cot = send(cotangent, ring(4))

    turned = context.T.reshape(4, quarter, tokens)
    moved = [
        send(
            at(turned, y ^ s),
            lambda x, h, y, l, c, s=s: (l, c, y ^ s, l ^ x, h),
        )
        for s in range(4)
    ]
    mine = jnp.stack(moved)
    own = jnp.stack(
        [mine]
        + [send(mine, lambda x, h, y, l, c, k=k: (x, h, y, l ^ k, c)) for k in (1, 2, 3)]
    )
    swap = lambda x, h, y, l, c: (x, h, y, l, 1 - c)
    other = send(own, swap)

    near_rows = gather_y(jnp.concatenate(gather_x(cotangent)))
    far_rows = gather_x(jnp.concatenate(gather_y(far_cot)))

    half = tokens // 2
    after = jnp.where(l == 3, far_cot, cotangent)
    before = jnp.where(l == 0, far_cot, cotangent)
    skip = jnp.concatenate(
        [
            jnp.where(l >= 2, far_cot[:half], cotangent[:half]),
            jnp.where(l <= 1, far_cot[half:], cotangent[half:]),
        ]
    )
    left = jnp.stack([cotangent, after, skip, before])
    blocks = (l + jnp.arange(4, dtype=jnp.int32)) % 4 * 2
    given = partial_products((blocks + 1 - c).astype(jnp.int32), left, out_weight)
    taken = send(given, swap)
    kept = partial_products((blocks + c).astype(jnp.int32), left, out_weight)
    both = [kept[i] + taken[i] for i in range(4)]
    from_before = send(both[1], ring(1))
    from_after = send(both[3], ring(-1))
    from_two_before = send(both[2][:half], ring(2))
    from_two_after = send(both[2][half:], ring(-2))
    grad_context = (
        both[0]
        + from_before
        + from_after
        + jnp.concatenate([from_two_before, from_two_after])
    ).astype(BF16)

    grad_weight = weight_gradient(
        jnp.stack([l, c ^ h]).astype(jnp.int32), own, other, near_rows + far_rows
    )
    return grad_weight, grad_context


def solution(mesh):
    return jax.shard_map(
        shards,
        mesh=mesh,
        in_specs=(P(("batch", "seq"), "mp"), P(("batch", "seq"), "mp"), P(None, "mp")),
        out_specs=(P(("batch", "seq"), "mp"), P(("batch", "seq"), "mp")),
        check_vma=False,
    )
```

```python
import functools

import jax
import jax.numpy as jnp
from jax import lax
from jax.experimental import pallas as pl
from jax.experimental.pallas import tpu as pltpu
from jax.sharding import PartitionSpec as P


AXES = ("batch", "seq", "mp")
F32 = jnp.float32
BF16 = jnp.bfloat16
VMEM = pl.BlockSpec(memory_space=pltpu.VMEM)
SMEM = pl.BlockSpec(memory_space=pltpu.SMEM)

GIVEN, KEPT, PICK, LOW, MIXED, CORE = 0, 8, 16, 24, 25, 26


def place(x, h, y, l, c):
    return ((x * 2 + h) * 4 + y) * 8 + l * 2 + c


def pairs(route):
    return [
        (place(x, h, y, l, c), place(*route(x, h, y, l, c)))
        for x in range(4)
        for h in range(2)
        for y in range(4)
        for l in range(4)
        for c in range(2)
    ]


def ring(step):
    def route(x, h, y, l, c):
        z = (4 * h + l + step) % 8
        return x, z // 4, y, z % 4, c

    return route


def crosswise(k, first):
    def route(x, h, y, l, c):
        if (c == 0) == first:
            return x ^ k, h, y, l, c
        return x, h, y ^ k, l, c

    return route


def send(array, route):
    return lax.ppermute(array, AXES, pairs(route))


def at(stack, index):
    return lax.dynamic_index_in_dim(stack, index, 0, keepdims=False)


def product(weight, near, far, use_far):
    right = jnp.where(use_far, far[...], near[...])
    return lax.dot_general(
        weight[...], right, (((1,), (1,)), ((), ())), preferred_element_type=F32
    )


def given_kernel(table, weight, near, far, out):
    i = pl.program_id(0)
    out[0] = product(weight, near, far, table[PICK + i] == 1)


def kept_kernel(table, weight, near, far, taken, here, after, before, skip_up, skip_down):
    i = pl.program_id(0)
    total = product(weight, near, far, table[PICK + i] == 1) + taken[0]
    for j, out in enumerate((here, after, before)):

        @pl.when(i // 2 == j)
        def _(out=out):
            out[...] = total

    for j, out in ((6, skip_up), (7, skip_down)):

        @pl.when(i == j)
        def _(out=out):
            out[...] = total


def products(start, table, weight, near, far, taken=None):
    tokens, depth = near.shape
    rows = depth // 2
    whole = pl.BlockSpec((tokens, depth), lambda i, t: (0, 0))
    specs = [pl.BlockSpec((rows, depth), lambda i, t: (t[start + i], 0)), whole, whole]
    step = pl.BlockSpec((1, rows, tokens), lambda i, t: (i, 0, 0))
    args = [table, weight, near, far]
    if taken is None:
        kernel, shapes, outs = given_kernel, jax.ShapeDtypeStruct((8, rows, tokens), F32), step
    else:
        kernel = kept_kernel
        specs.append(step)
        args.append(taken)
        shapes = [jax.ShapeDtypeStruct((n * rows, tokens), F32) for n in (2, 2, 2, 1, 1)]
        outs = [
            pl.BlockSpec((rows, tokens), lambda i, t, j=j: (jnp.clip(i - 2 * j, 0, 1), 0))
            for j in range(3)
        ] + [pl.BlockSpec((rows, tokens), lambda i, t: (0, 0))] * 2
    return pl.pallas_call(
        kernel,
        out_shape=shapes,
        grid_spec=pltpu.PrefetchScalarGridSpec(
            num_scalar_prefetch=1, grid=(8,), in_specs=specs, out_specs=outs
        ),
        cost_estimate=pl.CostEstimate(
            flops=16 * rows * tokens * depth,
            bytes_accessed=8 * rows * depth * 2 + 8 * rows * tokens * 4,
            transcendentals=0,
        ),
    )(*args)


def finish_kernel(here, before, after, two_before, two_after, out):
    rows = two_before.shape[0]
    for i, skip in enumerate((two_before, two_after)):
        part = pl.ds(i * rows, rows)
        total = here[part, :] + before[part, :] + after[part, :] + skip[...]
        out[:, part] = total.T.astype(BF16)


def weight_kernel(far, table, own, other, *refs):
    cots, out = refs[:4], refs[-1]
    low, core = table[LOW], table[CORE]
    use_own = table[MIXED] == far
    total = refs[4][...] if far else jnp.zeros(out.shape, F32)
    for piece, cot in enumerate(cots):
        for half in range(2):
            lefts = []
            for m in (2 * half, 2 * half + 1):
                r = jnp.where(core == 0, m, piece)
                s = jnp.where(core == 0, piece, m)
                k = low ^ r
                lefts.append(jnp.where(use_own, own[k, s], other[k, s]))
            left = jnp.concatenate(lefts, axis=1)
            right = cot[pl.ds(256 * half, 256), :]
            total += jnp.dot(left, right, preferred_element_type=F32)
    out[...] = total


def weight_part(far, table, own, other, cots, total=()):
    rows, width = own.shape[2], cots[0].shape[1]
    return pl.pallas_call(
        functools.partial(weight_kernel, far),
        out_shape=jax.ShapeDtypeStruct((rows, width), F32),
        in_specs=[SMEM] + [VMEM] * (6 + len(total)),
        out_specs=VMEM,
        cost_estimate=pl.CostEstimate(
            flops=2 * rows * width * 512 * 4,
            bytes_accessed=4 * 512 * width * 2,
            transcendentals=0,
        ),
    )(table, own, other, *cots, *total)


def scalars(h, l, c):
    relative = jnp.array([0, 0, 1, 1, 3, 3, 2, 2], jnp.int32)
    step = jnp.array([0, 0, 1, 1, -1, -1, 2, -2], jnp.int32)
    half = jnp.array([0, 1] * 4, jnp.int32)
    block = (l + relative) % 4 * 4 + half
    pick = ((4 * h + l + step + 8) % 8 // 4 != h).astype(jnp.int32)
    rest = jnp.stack([l, c ^ h, c])
    return jnp.concatenate([block + 2 * (1 - c), block + 2 * c, pick, rest]).astype(jnp.int32)


def step(context, cotangent, out_weight):
    batch, y, mp = (lax.axis_index(a) for a in AXES)
    h = batch % 2
    l, c = mp // 2, mp % 2
    tokens, width = cotangent.shape
    quarter = width // 4
    table = scalars(h, l, c)

    def gather(array):
        first = [array] + [send(array, crosswise(k, True)) for k in (1, 2, 3)]
        row = jnp.concatenate(first)
        return [row] + [send(row, crosswise(k, False)) for k in (1, 2, 3)]

    near_cots = gather(cotangent)
    far_cot = send(cotangent, ring(4))
    far_cots = gather(far_cot)

    turned = context.T.reshape(4, quarter, tokens)
    mine = jnp.stack(
        [
            send(at(turned, y ^ s), lambda x, h, y, l, c, s=s: (l, c, y ^ s, l ^ x, h))
            for s in range(4)
        ]
    )
    own = jnp.stack(
        [mine]
        + [send(mine, lambda x, h, y, l, c, k=k: (x, h, y, l ^ k, c)) for k in (1, 2, 3)]
    )
    swap = lambda x, h, y, l, c: (x, h, y, l, 1 - c)
    other = send(own, swap)

    given = products(GIVEN, table, out_weight, cotangent, far_cot)
    taken = send(given, swap)
    here, after, before, skip_up, skip_down = products(
        KEPT, table, out_weight, cotangent, far_cot, taken
    )
    from_before = send(after, ring(1))
    from_after = send(before, ring(-1))
    from_two_before = send(skip_up, ring(2))
    from_two_after = send(skip_down, ring(-2))

    near_part = weight_part(0, table, own, other, near_cots)
    grad_weight = weight_part(1, table, own, other, far_cots, (near_part,))
    grad_context = pl.pallas_call(
        finish_kernel,
        out_shape=jax.ShapeDtypeStruct((tokens, width), BF16),
        in_specs=[VMEM] * 5,
        out_specs=VMEM,
        cost_estimate=pl.CostEstimate(
            flops=4 * tokens * width, bytes_accessed=18 * tokens * width, transcendentals=0
        ),
    )(here, from_before, from_after, from_two_before, from_two_after)
    return grad_weight, grad_context


def solution(mesh):
    return jax.shard_map(
        step,
        mesh=mesh,
        in_specs=(P(("batch", "seq"), "mp"), P(("batch", "seq"), "mp"), P(None, "mp")),
        out_specs=(P(("batch", "seq"), "mp"), P(("batch", "seq"), "mp")),
        check_vma=False,
    )
```

```python
import functools

import jax
import jax.numpy as jnp
import numpy as np
from jax import lax
from jax.experimental import pallas as pl
from jax.experimental.pallas import tpu as pltpu
from jax.sharding import PartitionSpec as P


AXES = ("batch", "seq", "mp")
F32 = jnp.float32
BF16 = jnp.bfloat16
VMEM = pl.BlockSpec(memory_space=pltpu.VMEM)
SMEM = pl.BlockSpec(memory_space=pltpu.SMEM)

GIVEN, KEPT, PICK, LOW, MIXED, CORE = 0, 4, 8, 16, 17, 18


def place(x, h, y, l, c):
    return ((x * 2 + h) * 4 + y) * 8 + l * 2 + c


def pairs(route):
    return [
        (place(x, h, y, l, c), place(*route(x, h, y, l, c)))
        for x in range(4)
        for h in range(2)
        for y in range(4)
        for l in range(4)
        for c in range(2)
    ]


def ring(step):
    def route(x, h, y, l, c):
        z = (4 * h + l + step) % 8
        return x, z // 4, y, z % 4, c

    return route


def crosswise(k, first):
    def route(x, h, y, l, c):
        if (c == 0) == first:
            return x ^ k, h, y, l, c
        return x, h, y ^ k, l, c

    return route


def send(array, route):
    return lax.ppermute(array, AXES, pairs(route))


def at(stack, index):
    return lax.dynamic_index_in_dim(stack, index, 0, keepdims=False)


def turn(i, near, far, turned):
    @pl.when(i == 0)
    def _():
        turned[0] = near[...].T
        turned[1] = far[...].T


def product(table, i, weight, turned, half):
    rows = weight.shape[0] // 2
    return jnp.dot(
        weight[pl.ds(half * rows, rows), :],
        turned[table[PICK + 2 * i + half]],
        preferred_element_type=F32,
    )


def given_kernel(table, weight, near, far, out, turned):
    i = pl.program_id(0)
    turn(i, near, far, turned)
    rows = weight.shape[0] // 2
    for half in range(2):
        out[0, pl.ds(half * rows, rows), :] = product(table, i, weight, turned, half)


def kept_kernel(table, weight, near, far, taken, here, after, before, up, down, turned):
    i = pl.program_id(0)
    turn(i, near, far, turned)
    rows = weight.shape[0] // 2
    for half in range(2):
        part = pl.ds(half * rows, rows)
        total = product(table, i, weight, turned, half) + taken[0, part, :]
        for j, out in enumerate((here, after, before)):

            @pl.when(i == j)
            def _(out=out, part=part, total=total):
                out[part, :] = total

        @pl.when(i == 3)
        def _(out=(up, down)[half], total=total):
            out[...] = total


def products(start, table, weight, near, far, taken=None):
    tokens, depth = near.shape
    whole = pl.BlockSpec((tokens, depth), lambda i, t: (0, 0))
    specs = [pl.BlockSpec((depth, depth), lambda i, t: (t[start + i], 0)), whole, whole]
    block = pl.BlockSpec((1, depth, tokens), lambda i, t: (i, 0, 0))
    args = [table, weight, near, far]
    if taken is None:
        kernel, shapes, outs = given_kernel, jax.ShapeDtypeStruct((4, depth, tokens), F32), block
    else:
        kernel = kept_kernel
        specs.append(block)
        args.append(taken)
        rows = [depth, depth, depth, depth // 2, depth // 2]
        shapes = [jax.ShapeDtypeStruct((n, tokens), F32) for n in rows]
        outs = [pl.BlockSpec((n, tokens), lambda i, t: (0, 0)) for n in rows]
    return pl.pallas_call(
        kernel,
        out_shape=shapes,
        grid_spec=pltpu.PrefetchScalarGridSpec(
            num_scalar_prefetch=1,
            grid=(4,),
            in_specs=specs,
            out_specs=outs,
            scratch_shapes=[pltpu.VMEM((2, depth, tokens), BF16)],
        ),
        cost_estimate=pl.CostEstimate(
            flops=8 * depth * tokens * depth,
            bytes_accessed=8 * depth * depth + 16 * depth * tokens,
            transcendentals=0,
        ),
    )(*args)


def finish_kernel(here, before, after, two_before, two_after, out):
    rows = two_before.shape[0]
    for i, skip in enumerate((two_before, two_after)):
        part = pl.ds(i * rows, rows)
        total = here[part, :] + before[part, :] + after[part, :] + skip[...]
        out[:, part] = total.T.astype(BF16)


def weight_kernel(far, table, own, other, *refs):
    cots, out = refs[:4], refs[-1]
    low, core = table[LOW], table[CORE]
    use_own = table[MIXED] == far
    total = refs[4][...] if far else jnp.zeros(out.shape, F32)
    for piece, cot in enumerate(cots):
        for half in range(2):
            lefts = []
            for m in (2 * half, 2 * half + 1):
                r = jnp.where(core == 0, m, piece)
                s = jnp.where(core == 0, piece, m)
                k = low ^ r
                lefts.append(jnp.where(use_own, own[k, s], other[k, s]))
            left = jnp.concatenate(lefts, axis=1)
            right = cot[pl.ds(256 * half, 256), :]
            total += jnp.dot(left, right, preferred_element_type=F32)
    out[...] = total


def weight_part(far, table, own, other, cots, total=()):
    rows, width = own.shape[2], cots[0].shape[1]
    return pl.pallas_call(
        functools.partial(weight_kernel, far),
        out_shape=jax.ShapeDtypeStruct((rows, width), F32),
        in_specs=[SMEM] + [VMEM] * (6 + len(total)),
        out_specs=VMEM,
        cost_estimate=pl.CostEstimate(
            flops=2 * rows * width * 512 * 4,
            bytes_accessed=4 * 512 * width * 2,
            transcendentals=0,
        ),
    )(table, own, other, *cots, *total)


def scalars(device):
    rows = []
    for _ in range(4):
        for h in range(2):
            for _ in range(4):
                for l in range(4):
                    for c in range(2):
                        block = [(l + r) % 4 * 2 for r in (0, 1, 3, 2)]
                        step = (0, 0, 1, 1, -1, -1, 2, -2)
                        pick = [int((4 * h + l + d) % 8 // 4 != h) for d in step]
                        given = [b + 1 - c for b in block]
                        kept = [b + c for b in block]
                        rows.append(given + kept + pick + [l, c ^ h, c, 0, 0, 0, 0, 0])
    return at(jnp.asarray(np.array(rows, np.int32)), device)


def step(context, cotangent, out_weight):
    batch, y, mp = (lax.axis_index(a) for a in AXES)
    tokens, width = cotangent.shape
    quarter = width // 4
    table = scalars((batch * 4 + y) * 8 + mp)

    def gather(array):
        first = [array] + [send(array, crosswise(k, True)) for k in (1, 2, 3)]
        row = jnp.concatenate(first)
        return [row] + [send(row, crosswise(k, False)) for k in (1, 2, 3)]

    near_cots = gather(cotangent)
    far_cot = send(cotangent, ring(4))
    far_cots = gather(far_cot)

    block = send(context, lambda x, h, y, l, c: (l, c, y, l ^ x, h))
    turned = block.T.reshape(4, quarter, tokens)
    mine = jnp.stack(
        [at(turned, y)]
        + [
            send(at(turned, y ^ k), lambda x, h, y, l, c, k=k: (x, h, y ^ k, l, c))
            for k in (1, 2, 3)
        ]
    )
    own = jnp.stack(
        [mine]
        + [send(mine, lambda x, h, y, l, c, k=k: (x, h, y, l ^ k, c)) for k in (1, 2, 3)]
    )
    swap = lambda x, h, y, l, c: (x, h, y, l, 1 - c)
    other = send(own, swap)

    given = products(GIVEN, table, out_weight, cotangent, far_cot)
    taken = send(given, swap)
    here, after, before, skip_up, skip_down = products(
        KEPT, table, out_weight, cotangent, far_cot, taken
    )
    from_before = send(after, ring(1))
    from_after = send(before, ring(-1))
    from_two_before = send(skip_up, ring(2))
    from_two_after = send(skip_down, ring(-2))

    near_part = weight_part(0, table, own, other, near_cots)
    grad_weight = weight_part(1, table, own, other, far_cots, (near_part,))
    grad_context = pl.pallas_call(
        finish_kernel,
        out_shape=jax.ShapeDtypeStruct((tokens, width), BF16),
        in_specs=[VMEM] * 5,
        out_specs=VMEM,
        cost_estimate=pl.CostEstimate(
            flops=4 * tokens * width, bytes_accessed=18 * tokens * width, transcendentals=0
        ),
    )(here, from_before, from_after, from_two_before, from_two_after)
    return grad_weight, grad_context


def solution(mesh):
    return jax.shard_map(
        step,
        mesh=mesh,
        in_specs=(P(("batch", "seq"), "mp"), P(("batch", "seq"), "mp"), P(None, "mp")),
        out_specs=(P(("batch", "seq"), "mp"), P(("batch", "seq"), "mp")),
        check_vma=False,
    )
```

```python
import functools

import jax
import jax.numpy as jnp
from jax import lax
from jax.experimental import pallas as pl
from jax.experimental.pallas import tpu as pltpu
from jax.sharding import PartitionSpec as P


AXES = ("batch", "seq", "mp")
F32 = jnp.float32
BF16 = jnp.bfloat16
VMEM = pl.BlockSpec(memory_space=pltpu.VMEM)

MIB = 1 << 20


def here():
    batch, mp = lax.axis_index("batch"), lax.axis_index("mp")
    return batch & 1, mp >> 1, mp & 1


def place(x, h, y, l, c):
    return ((x * 2 + h) * 4 + y) * 8 + l * 2 + c


def pairs(route):
    return [
        (place(x, h, y, l, c), place(*route(x, h, y, l, c)))
        for x in range(4)
        for h in range(2)
        for y in range(4)
        for l in range(4)
        for c in range(2)
    ]


def ring(step):
    def route(x, h, y, l, c):
        z = (4 * h + l + step) % 8
        return x, z // 4, y, z % 4, c

    return route


def crosswise(k, first):
    def route(x, h, y, l, c):
        if (c == 0) == first:
            return x ^ k, h, y, l, c
        return x, h, y ^ k, l, c

    return route


def send(array, route):
    return lax.ppermute(array, AXES, pairs(route))


def at(stack, index):
    return lax.dynamic_index_in_dim(stack, index, 0, keepdims=False)


def products_kernel(kept, weight, near, far, *refs):
    h, l, c = here()
    turned = refs[-1]
    turned[0] = near[...].T
    turned[1] = far[...].T
    depth = near.shape[1]
    rows = depth // 2
    core = c if kept else 1 - c
    for i, (block, steps) in enumerate(((0, (0, 0)), (1, (1, 1)), (3, (-1, -1)), (2, (2, -2)))):
        for half, step in enumerate(steps):
            target = (4 * h + l + step + 8) & 7
            use_far = (target >> 2) ^ h
            row = ((((l + block) & 3) * 2 + core) * 2 + half) * rows
            part = pl.ds(half * rows, rows)
            total = jnp.dot(
                weight[pl.ds(pl.multiple_of(row, rows), rows), :],
                turned[use_far],
                preferred_element_type=F32,
            )
            if not kept:
                refs[0][i, part, :] = total
                continue
            total += refs[0][i, part, :]
            if i < 3:
                refs[1 + i][part, :] = total
            else:
                refs[4 + half][...] = total


def products(weight, near, far, *taken):
    tokens, depth = near.shape
    kept = bool(taken)
    if kept:
        rows = [depth, depth, depth, depth // 2, depth // 2]
        shapes = [jax.ShapeDtypeStruct((n, tokens), F32) for n in rows]
    else:
        shapes = [jax.ShapeDtypeStruct((4, depth, tokens), F32)]
    return pl.pallas_call(
        functools.partial(products_kernel, kept),
        out_shape=shapes,
        in_specs=[VMEM] * (3 + kept),
        out_specs=[VMEM] * len(shapes),
        scratch_shapes=[pltpu.VMEM((2, depth, tokens), BF16)],
        compiler_params=pltpu.CompilerParams(vmem_limit_bytes=20 * MIB),
        cost_estimate=pl.CostEstimate(
            flops=8 * depth * tokens * depth,
            bytes_accessed=8 * depth * depth + 16 * depth * tokens,
            transcendentals=0,
        ),
    )(weight, near, far, *taken)


def finish_kernel(home, before, after, two_before, two_after, out):
    rows = two_before.shape[0]
    for i, skip in enumerate((two_before, two_after)):
        part = pl.ds(i * rows, rows)
        total = home[part, :] + before[part, :] + after[part, :] + skip[...]
        out[:, part] = total.T.astype(BF16)


def weight_kernel(far, own, other, *refs):
    h, low, core = here()
    cots, out = refs[:4], refs[-1]
    use_own = (core ^ h) == far
    total = refs[4][...] if far else jnp.zeros(out.shape, F32)
    for piece, cot in enumerate(cots):
        for half in range(2):
            lefts = []
            for m in (2 * half, 2 * half + 1):
                r = jnp.where(core == 0, m, piece)
                s = jnp.where(core == 0, piece, m)
                k = low ^ r
                lefts.append(jnp.where(use_own, own[k, s], other[k, s]))
            left = jnp.concatenate(lefts, axis=1)
            right = cot[pl.ds(256 * half, 256), :]
            total += jnp.dot(left, right, preferred_element_type=F32)
    out[...] = total


def weight_part(far, own, other, cots, *total):
    rows, width = own.shape[2], cots[0].shape[1]
    return pl.pallas_call(
        functools.partial(weight_kernel, far),
        out_shape=jax.ShapeDtypeStruct((rows, width), F32),
        in_specs=[VMEM] * (6 + len(total)),
        out_specs=VMEM,
        compiler_params=pltpu.CompilerParams(vmem_limit_bytes=16 * MIB),
        cost_estimate=pl.CostEstimate(
            flops=2 * rows * width * 512 * 4,
            bytes_accessed=4 * 512 * width * 2,
            transcendentals=0,
        ),
    )(own, other, *cots, *total)


def step(context, cotangent, out_weight):
    y = lax.axis_index("seq")
    tokens, width = cotangent.shape
    quarter = width // 4

    def gather(array):
        first = [array] + [send(array, crosswise(k, True)) for k in (1, 2, 3)]
        row = jnp.concatenate(first)
        return [row] + [send(row, crosswise(k, False)) for k in (1, 2, 3)]

    near_cots = gather(cotangent)
    far_cot = send(cotangent, ring(4))
    far_cots = gather(far_cot)

    turned = context.T.reshape(4, quarter, tokens)
    block = jnp.stack(
        [at(turned, y)]
        + [
            send(at(turned, y ^ k), lambda x, h, y, l, c, k=k: (x, h, y ^ k, l, c))
            for k in (1, 2, 3)
        ]
    )
    mine = send(block, lambda x, h, y, l, c: (l, c, y, l ^ x, h))
    gathered = [mine] + [
        send(mine, lambda x, h, y, l, c, k=k: (x, h, y, l ^ k, c)) for k in (1, 2, 3)
    ]
    own = jnp.stack(gathered)
    swap = lambda x, h, y, l, c: (x, h, y, l, 1 - c)
    other = send(own, swap)

    (given,) = products(out_weight, cotangent, far_cot)
    taken = send(given, swap)
    at_home, after, before, skip_up, skip_down = products(out_weight, cotangent, far_cot, taken)
    from_before = send(after, ring(1))
    from_after = send(before, ring(-1))
    from_two_before = send(skip_up, ring(2))
    from_two_after = send(skip_down, ring(-2))

    near_part = weight_part(0, own, other, near_cots)
    grad_weight = weight_part(1, own, other, far_cots, near_part)
    grad_context = pl.pallas_call(
        finish_kernel,
        out_shape=jax.ShapeDtypeStruct((tokens, width), BF16),
        in_specs=[VMEM] * 5,
        out_specs=VMEM,
        compiler_params=pltpu.CompilerParams(vmem_limit_bytes=8 * MIB),
        cost_estimate=pl.CostEstimate(
            flops=4 * tokens * width, bytes_accessed=18 * tokens * width, transcendentals=0
        ),
    )(at_home, from_before, from_after, from_two_before, from_two_after)
    return grad_weight, grad_context


def solution(mesh):
    return jax.shard_map(
        step,
        mesh=mesh,
        in_specs=(P(("batch", "seq"), "mp"), P(("batch", "seq"), "mp"), P(None, "mp")),
        out_specs=(P(("batch", "seq"), "mp"), P(("batch", "seq"), "mp")),
        check_vma=False,
    )
```

```python
import functools

import jax
import jax.numpy as jnp
from jax import lax
from jax.experimental import pallas as pl
from jax.experimental.pallas import tpu as pltpu
from jax.sharding import PartitionSpec as P


AXES = ("batch", "seq", "mp")
F32 = jnp.float32
BF16 = jnp.bfloat16
VMEM = pl.BlockSpec(memory_space=pltpu.VMEM)

MIB = 1 << 20


def here():
    batch, mp = lax.axis_index("batch"), lax.axis_index("mp")
    return batch & 1, mp >> 1, mp & 1


def place(x, h, y, l, c):
    return ((x * 2 + h) * 4 + y) * 8 + l * 2 + c


def pairs(route):
    return [
        (place(x, h, y, l, c), place(*route(x, h, y, l, c)))
        for x in range(4)
        for h in range(2)
        for y in range(4)
        for l in range(4)
        for c in range(2)
    ]


def ring(step):
    def route(x, h, y, l, c):
        z = (4 * h + l + step) % 8
        return x, z // 4, y, z % 4, c

    return route


def crosswise(k, first):
    def route(x, h, y, l, c):
        if (c == 0) == first:
            return x ^ k, h, y, l, c
        return x, h, y ^ k, l, c

    return route


def send(array, route):
    return lax.ppermute(array, AXES, pairs(route))


def at(stack, index):
    return lax.dynamic_index_in_dim(stack, index, 0, keepdims=False)


def products_kernel(kept, weight, near, far, *refs):
    h, l, c = here()
    turned, blocks, arrived = refs[-3:]
    depth = near.shape[1]
    rows = depth // 2
    core = c if kept else 1 - c
    copies = []
    for i, block in enumerate((0, 1, 3, 2)):
        for half in range(2):
            row = ((((l + block) & 3) * 2 + core) * 2 + half) * rows
            copies.append(
                pltpu.make_async_copy(
                    weight.at[pl.ds(pl.multiple_of(row, rows), rows), :],
                    blocks.at[i, half],
                    arrived.at[i, half],
                )
            )
            copies[-1].start()
    turned[0] = near[...].T
    turned[1] = far[...].T
    for i, steps in enumerate(((0, 0), (1, 1), (-1, -1), (2, -2))):
        for half, step in enumerate(steps):
            target = (4 * h + l + step + 8) & 7
            use_far = (target >> 2) ^ h
            part = pl.ds(half * rows, rows)
            copies[2 * i + half].wait()
            total = jnp.dot(
                blocks[i, half], turned[use_far], preferred_element_type=F32
            )
            if not kept:
                refs[0][i, part, :] = total
                continue
            total += refs[0][i, part, :]
            if i < 3:
                refs[1 + i][part, :] = total
            else:
                refs[4 + half][...] = total


def products(weight, near, far, *taken):
    tokens, depth = near.shape
    kept = bool(taken)
    if kept:
        rows = [depth, depth, depth, depth // 2, depth // 2]
        shapes = [jax.ShapeDtypeStruct((n, tokens), F32) for n in rows]
    else:
        shapes = [jax.ShapeDtypeStruct((4, depth, tokens), F32)]
    return pl.pallas_call(
        functools.partial(products_kernel, kept),
        out_shape=shapes,
        in_specs=[pl.BlockSpec(memory_space=pltpu.HBM)] + [VMEM] * (2 + kept),
        out_specs=[VMEM] * len(shapes),
        scratch_shapes=[
            pltpu.VMEM((2, depth, tokens), BF16),
            pltpu.VMEM((4, 2, depth // 2, depth), BF16),
            pltpu.SemaphoreType.DMA((4, 2)),
        ],
        compiler_params=pltpu.CompilerParams(vmem_limit_bytes=48 * MIB),
        cost_estimate=pl.CostEstimate(
            flops=8 * depth * tokens * depth,
            bytes_accessed=8 * depth * depth + 16 * depth * tokens,
            transcendentals=0,
        ),
    )(weight, near, far, *taken)


def finish_kernel(home, before, after, two_before, two_after, out):
    rows = two_before.shape[0]
    for i, skip in enumerate((two_before, two_after)):
        part = pl.ds(i * rows, rows)
        total = home[part, :] + before[part, :] + after[part, :] + skip[...]
        out[:, part] = total.T.astype(BF16)


def weight_kernel(far, own, other, *refs):
    h, low, core = here()
    cots, out = refs[:4], refs[-1]
    use_own = (core ^ h) == far
    total = refs[4][...] if far else jnp.zeros(out.shape, F32)
    for piece, cot in enumerate(cots):
        for half in range(2):
            lefts = []
            for m in (2 * half, 2 * half + 1):
                r = jnp.where(core == 0, m, piece)
                s = jnp.where(core == 0, piece, m)
                k = low ^ r
                lefts.append(jnp.where(use_own, own[k, s], other[k, s]))
            left = jnp.concatenate(lefts, axis=1)
            right = cot[pl.ds(256 * half, 256), :]
            total += jnp.dot(left, right, preferred_element_type=F32)
    out[...] = total


def weight_part(far, own, other, cots, *total):
    rows, width = own.shape[2], cots[0].shape[1]
    return pl.pallas_call(
        functools.partial(weight_kernel, far),
        out_shape=jax.ShapeDtypeStruct((rows, width), F32),
        in_specs=[VMEM] * (6 + len(total)),
        out_specs=VMEM,
        compiler_params=pltpu.CompilerParams(vmem_limit_bytes=16 * MIB),
        cost_estimate=pl.CostEstimate(
            flops=2 * rows * width * 512 * 4,
            bytes_accessed=4 * 512 * width * 2,
            transcendentals=0,
        ),
    )(own, other, *cots, *total)


def step(context, cotangent, out_weight):
    y = lax.axis_index("seq")
    tokens, width = cotangent.shape
    quarter = width // 4

    def gather(array):
        first = [array] + [send(array, crosswise(k, True)) for k in (1, 2, 3)]
        row = jnp.concatenate(first)
        return [row] + [send(row, crosswise(k, False)) for k in (1, 2, 3)]

    near_cots = gather(cotangent)
    far_cot = send(cotangent, ring(4))
    far_cots = gather(far_cot)

    turned = context.T.reshape(4, quarter, tokens)
    block = jnp.stack(
        [at(turned, y)]
        + [
            send(at(turned, y ^ k), lambda x, h, y, l, c, k=k: (x, h, y ^ k, l, c))
            for k in (1, 2, 3)
        ]
    )
    mine = send(block, lambda x, h, y, l, c: (l, c, y, l ^ x, h))
    gathered = [mine] + [
        send(mine, lambda x, h, y, l, c, k=k: (x, h, y, l ^ k, c)) for k in (1, 2, 3)
    ]
    own = jnp.stack(gathered)
    swap = lambda x, h, y, l, c: (x, h, y, l, 1 - c)
    other = send(own, swap)

    (given,) = products(out_weight, cotangent, far_cot)
    taken = send(given, swap)
    at_home, after, before, skip_up, skip_down = products(out_weight, cotangent, far_cot, taken)
    from_before = send(after, ring(1))
    from_after = send(before, ring(-1))
    from_two_before = send(skip_up, ring(2))
    from_two_after = send(skip_down, ring(-2))

    near_part = weight_part(0, own, other, near_cots)
    grad_weight = weight_part(1, own, other, far_cots, near_part)
    grad_context = pl.pallas_call(
        finish_kernel,
        out_shape=jax.ShapeDtypeStruct((tokens, width), BF16),
        in_specs=[VMEM] * 5,
        out_specs=VMEM,
        compiler_params=pltpu.CompilerParams(vmem_limit_bytes=8 * MIB),
        cost_estimate=pl.CostEstimate(
            flops=4 * tokens * width, bytes_accessed=18 * tokens * width, transcendentals=0
        ),
    )(at_home, from_before, from_after, from_two_before, from_two_after)
    return grad_weight, grad_context


def solution(mesh):
    return jax.shard_map(
        step,
        mesh=mesh,
        in_specs=(P(("batch", "seq"), "mp"), P(("batch", "seq"), "mp"), P(None, "mp")),
        out_specs=(P(("batch", "seq"), "mp"), P(("batch", "seq"), "mp")),
        check_vma=False,
    )
```

```python
import functools

import jax
import jax.numpy as jnp
from jax import lax
from jax.experimental import pallas as pl
from jax.experimental.pallas import tpu as pltpu
from jax.sharding import PartitionSpec as P


AXES = ("batch", "seq", "mp")
F32 = jnp.float32
BF16 = jnp.bfloat16
VMEM = pl.BlockSpec(memory_space=pltpu.VMEM)

MIB = 1 << 20


def here():
    batch, mp = lax.axis_index("batch"), lax.axis_index("mp")
    return batch & 1, mp >> 1, mp & 1


def place(x, h, y, l, c):
    return ((x * 2 + h) * 4 + y) * 8 + l * 2 + c


def pairs(route):
    return [
        (place(x, h, y, l, c), place(*route(x, h, y, l, c)))
        for x in range(4)
        for h in range(2)
        for y in range(4)
        for l in range(4)
        for c in range(2)
    ]


def ring(step):
    def route(x, h, y, l, c):
        z = (4 * h + l + step) % 8
        return x, z // 4, y, z % 4, c

    return route


def crosswise(k, first):
    def route(x, h, y, l, c):
        if (c == 0) == first:
            return x ^ k, h, y, l, c
        return x, h, y ^ k, l, c

    return route


def send(array, route):
    return lax.ppermute(array, AXES, pairs(route))


def at(stack, index):
    return lax.dynamic_index_in_dim(stack, index, 0, keepdims=False)


def products_kernel(kept, weight, near, far, *refs):
    h, l, c = here()
    turned = refs[-1]
    turned[0] = near[...].T
    turned[1] = far[...].T
    depth = near.shape[1]
    rows = depth // 2
    core = c if kept else 1 - c
    for i, (block, steps) in enumerate(((0, (0, 0)), (1, (1, 1)), (3, (-1, -1)), (2, (2, -2)))):
        for half, step in enumerate(steps):
            target = (4 * h + l + step + 8) & 7
            use_far = (target >> 2) ^ h
            row = ((((l + block) & 3) * 2 + core) * 2 + half) * rows
            part = pl.ds(half * rows, rows)
            total = jnp.dot(
                weight[pl.ds(pl.multiple_of(row, rows), rows), :],
                turned[use_far],
                preferred_element_type=F32,
            )
            if not kept:
                refs[0][i, part, :] = total
                continue
            total += refs[0][i, part, :]
            if i < 3:
                refs[1 + i][part, :] = total
            else:
                refs[4 + half][...] = total


def products(weight, near, far, *taken):
    tokens, depth = near.shape
    kept = bool(taken)
    if kept:
        rows = [depth, depth, depth, depth // 2, depth // 2]
        shapes = [jax.ShapeDtypeStruct((n, tokens), F32) for n in rows]
    else:
        shapes = [jax.ShapeDtypeStruct((4, depth, tokens), F32)]
    return pl.pallas_call(
        functools.partial(products_kernel, kept),
        out_shape=shapes,
        in_specs=[VMEM] * (3 + kept),
        out_specs=[VMEM] * len(shapes),
        scratch_shapes=[pltpu.VMEM((2, depth, tokens), BF16)],
        compiler_params=pltpu.CompilerParams(vmem_limit_bytes=20 * MIB),
        cost_estimate=pl.CostEstimate(
            flops=8 * depth * tokens * depth,
            bytes_accessed=8 * depth * depth + 16 * depth * tokens,
            transcendentals=0,
        ),
    )(weight, near, far, *taken)


def finish_kernel(home, before, after, two_before, two_after, out):
    rows = two_before.shape[0]
    for i, skip in enumerate((two_before, two_after)):
        part = pl.ds(i * rows, rows)
        total = home[part, :] + before[part, :] + after[part, :] + skip[...]
        out[:, part] = total.T.astype(BF16)


def weight_kernel(items, own, other, *refs):
    h, low, core = here()
    swapped = core != h
    arrays = max(a for a, _, _, _ in items) + 1
    out = refs[-1]
    total = refs[arrays][...] if len(refs) > arrays + 1 else jnp.zeros(out.shape, F32)
    for a, row, i, j in items:
        r = jnp.where(core == 0, i, j)
        s = jnp.where(core == 0, j, i)
        mine, theirs = own[low ^ r, s], other[low ^ r, s]
        near = jnp.where(swapped, theirs, mine)
        far = jnp.where(swapped, mine, theirs)
        left = jnp.concatenate([near, far], axis=1)
        right = refs[a][pl.ds(row, left.shape[1]), :]
        total += jnp.dot(left, right, preferred_element_type=F32)
    out[...] = total


def weight_part(items, own, other, arrays, *total):
    rows, width = own.shape[2], arrays[0].shape[1]
    depth = 2 * own.shape[3] * len(items)
    return pl.pallas_call(
        functools.partial(weight_kernel, items),
        out_shape=jax.ShapeDtypeStruct((rows, width), F32),
        in_specs=[VMEM] * (2 + len(arrays) + len(total)),
        out_specs=VMEM,
        compiler_params=pltpu.CompilerParams(vmem_limit_bytes=16 * MIB),
        cost_estimate=pl.CostEstimate(
            flops=2 * rows * width * depth,
            bytes_accessed=2 * depth * (width + rows) + 8 * rows * width,
            transcendentals=0,
        ),
    )(own, other, *arrays, *total)


def step(context, cotangent, out_weight):
    y = lax.axis_index("seq")
    tokens, width = cotangent.shape
    quarter = width // 4

    others = (1, 2, 3)

    far_cot = send(cotangent, ring(4))
    pair = jnp.concatenate([cotangent, far_cot])
    first = [send(pair, crosswise(k, True)) for k in others]
    second = [send(pair, crosswise(k, False)) for k in others]
    row = jnp.concatenate(first)
    both = [send(row, crosswise(k, False)) for k in others]

    turned = context.T.reshape(4, quarter, tokens)
    block = jnp.stack(
        [at(turned, y)]
        + [
            send(at(turned, y ^ k), lambda x, h, y, l, c, k=k: (x, h, y ^ k, l, c))
            for k in (1, 2, 3)
        ]
    )
    mine = send(block, lambda x, h, y, l, c: (l, c, y, l ^ x, h))
    gathered = [mine] + [
        send(mine, lambda x, h, y, l, c, k=k: (x, h, y, l ^ k, c)) for k in (1, 2, 3)
    ]
    own = jnp.stack(gathered)
    swap = lambda x, h, y, l, c: (x, h, y, l, 1 - c)
    other = send(own, swap)

    (given,) = products(out_weight, cotangent, far_cot)
    taken = send(given, swap)
    at_home, after, before, skip_up, skip_down = products(out_weight, cotangent, far_cot, taken)
    from_before = send(after, ring(1))
    from_after = send(before, ring(-1))
    from_two_before = send(skip_up, ring(2))
    from_two_after = send(skip_down, ring(-2))

    deep = 2 * tokens
    early = [(0, 0, 0, 0)] + [(k, 0, k, 0) for k in others] + [(3 + k, 0, 0, k) for k in others]
    late = [(k - 1, deep * (i - 1), i, k) for k in others for i in others]
    early_part = weight_part(early, own, other, [pair] + first + second)
    grad_weight = weight_part(late, own, other, both, early_part)
    grad_context = pl.pallas_call(
        finish_kernel,
        out_shape=jax.ShapeDtypeStruct((tokens, width), BF16),
        in_specs=[VMEM] * 5,
        out_specs=VMEM,
        compiler_params=pltpu.CompilerParams(vmem_limit_bytes=8 * MIB),
        cost_estimate=pl.CostEstimate(
            flops=4 * tokens * width, bytes_accessed=18 * tokens * width, transcendentals=0
        ),
    )(at_home, from_before, from_after, from_two_before, from_two_after)
    return grad_weight, grad_context


def solution(mesh):
    return jax.shard_map(
        step,
        mesh=mesh,
        in_specs=(P(("batch", "seq"), "mp"), P(("batch", "seq"), "mp"), P(None, "mp")),
        out_specs=(P(("batch", "seq"), "mp"), P(("batch", "seq"), "mp")),
        check_vma=False,
    )
```

```python
import functools

import jax
import jax.numpy as jnp
from jax import lax
from jax.experimental import pallas as pl
from jax.experimental.pallas import tpu as pltpu
from jax.sharding import PartitionSpec as P


AXES = ("batch", "seq", "mp")
F32 = jnp.float32
BF16 = jnp.bfloat16
VMEM = pl.BlockSpec(memory_space=pltpu.VMEM)

MIB = 1 << 20


def here():
    batch, mp = lax.axis_index("batch"), lax.axis_index("mp")
    return batch & 1, mp >> 1, mp & 1


def place(x, h, y, l, c):
    return ((x * 2 + h) * 4 + y) * 8 + l * 2 + c


def pairs(route):
    return [
        (place(x, h, y, l, c), place(*route(x, h, y, l, c)))
        for x in range(4)
        for h in range(2)
        for y in range(4)
        for l in range(4)
        for c in range(2)
    ]


def ring(step):
    def route(x, h, y, l, c):
        z = (4 * h + l + step) % 8
        return x, z // 4, y, z % 4, c

    return route


def crosswise(k, first):
    def route(x, h, y, l, c):
        if (c == 0) == first:
            return x ^ k, h, y, l, c
        return x, h, y ^ k, l, c

    return route


def send(array, route):
    return lax.ppermute(array, AXES, pairs(route))


def products_kernel(kept, weight, near, far, *refs):
    h, l, c = here()
    turned = refs[-1]
    turned[0] = near[...].T
    turned[1] = far[...].T
    depth = near.shape[1]
    rows = depth // 2
    core = c if kept else 1 - c
    for i, (block, steps) in enumerate(((0, (0, 0)), (1, (1, 1)), (3, (-1, -1)), (2, (2, -2)))):
        for half, step in enumerate(steps):
            target = (4 * h + l + step + 8) & 7
            use_far = (target >> 2) ^ h
            row = ((((l + block) & 3) * 2 + core) * 2 + half) * rows
            part = pl.ds(half * rows, rows)
            total = jnp.dot(
                weight[pl.ds(pl.multiple_of(row, rows), rows), :],
                turned[use_far],
                preferred_element_type=F32,
            )
            if not kept:
                refs[0][i, part, :] = total
                continue
            total += refs[0][i, part, :]
            if i < 3:
                refs[1 + i][part, :] = total
            else:
                refs[4 + half][...] = total


def products(weight, near, far, *taken):
    tokens, depth = near.shape
    kept = bool(taken)
    if kept:
        rows = [depth, depth, depth, depth // 2, depth // 2]
        shapes = [jax.ShapeDtypeStruct((n, tokens), F32) for n in rows]
    else:
        shapes = [jax.ShapeDtypeStruct((4, depth, tokens), F32)]
    return pl.pallas_call(
        functools.partial(products_kernel, kept),
        out_shape=shapes,
        in_specs=[VMEM] * (3 + kept),
        out_specs=[VMEM] * len(shapes),
        scratch_shapes=[pltpu.VMEM((2, depth, tokens), BF16)],
        compiler_params=pltpu.CompilerParams(vmem_limit_bytes=20 * MIB),
        cost_estimate=pl.CostEstimate(
            flops=8 * depth * tokens * depth,
            bytes_accessed=8 * depth * depth + 16 * depth * tokens,
            transcendentals=0,
        ),
    )(weight, near, far, *taken)


def finish_kernel(home, before, after, two_before, two_after, out):
    rows = two_before.shape[0]
    for i, skip in enumerate((two_before, two_after)):
        part = pl.ds(i * rows, rows)
        total = home[part, :] + before[part, :] + after[part, :] + skip[...]
        out[:, part] = total.T.astype(BF16)


def weight_kernel(items, own, other, *refs):
    h, low, core = here()
    swapped = core != h
    y = lax.axis_index("seq")
    arrays = 1 + max(max(item[0], item[2]) for item in items)
    tokens = own.shape[3]
    out = refs[-1]
    total = refs[arrays][...] if len(refs) > arrays + 1 else jnp.zeros(out.shape, F32)
    for a, row, b, far_row, i, j in items:
        k = low ^ jnp.where(core == 0, i, j)
        s = y ^ jnp.where(core == 0, j, i)
        mine, theirs = own[k, s], other[k, s]
        near = jnp.where(swapped, theirs, mine)
        far = jnp.where(swapped, mine, theirs)
        left = jnp.concatenate([near, far], axis=1)
        right = jnp.concatenate(
            [refs[a][pl.ds(row, tokens), :], refs[b][pl.ds(far_row, tokens), :]]
        )
        total += jnp.dot(left, right, preferred_element_type=F32)
    out[...] = total


def weight_part(items, own, other, arrays, *total):
    rows, width = own.shape[2], arrays[0].shape[1]
    depth = 2 * own.shape[3] * len(items)
    return pl.pallas_call(
        functools.partial(weight_kernel, items),
        out_shape=jax.ShapeDtypeStruct((rows, width), F32),
        in_specs=[VMEM] * (2 + len(arrays) + len(total)),
        out_specs=VMEM,
        compiler_params=pltpu.CompilerParams(vmem_limit_bytes=16 * MIB),
        cost_estimate=pl.CostEstimate(
            flops=2 * rows * width * depth,
            bytes_accessed=2 * depth * (width + rows) + 8 * rows * width,
            transcendentals=0,
        ),
    )(own, other, *arrays, *total)


def step(context, cotangent, out_weight):
    tokens, width = cotangent.shape
    quarter = width // 4

    others = (1, 2, 3)

    far_cot = send(cotangent, ring(4))
    pair = jnp.concatenate([cotangent, far_cot])
    first = [send(pair, crosswise(k, True)) for k in others]
    second = [send(cotangent, crosswise(k, False)) for k in others]
    row = jnp.concatenate([*first, far_cot])
    both = [send(row, crosswise(k, False)) for k in others]

    turned = context.T.reshape(4, quarter, tokens)
    block = lax.all_to_all(turned, "seq", split_axis=0, concat_axis=0, tiled=True)
    mine = send(block, lambda x, h, y, l, c: (l, c, y, l ^ x, h))
    gathered = [mine] + [
        send(mine, lambda x, h, y, l, c, k=k: (x, h, y, l ^ k, c)) for k in (1, 2, 3)
    ]
    own = jnp.stack(gathered)
    swap = lambda x, h, y, l, c: (x, h, y, l, 1 - c)
    other = send(own, swap)

    (given,) = products(out_weight, cotangent, far_cot)
    taken = send(given, swap)
    at_home, after, before, skip_up, skip_down = products(out_weight, cotangent, far_cot, taken)
    from_before = send(after, ring(1))
    from_after = send(before, ring(-1))
    from_two_before = send(skip_up, ring(2))
    from_two_after = send(skip_down, ring(-2))

    early = [(k, 0, k, tokens, k, 0) for k in range(4)]
    late = [(2 + k, 0, k - 1, 6 * tokens, 0, k) for k in others] + [
        (k - 1, 2 * tokens * (i - 1), k - 1, 2 * tokens * (i - 1) + tokens, i, k)
        for k in others
        for i in others
    ]
    early_part = weight_part(early, own, other, [pair] + first)
    grad_weight = weight_part(late, own, other, both + second, early_part)
    grad_context = pl.pallas_call(
        finish_kernel,
        out_shape=jax.ShapeDtypeStruct((tokens, width), BF16),
        in_specs=[VMEM] * 5,
        out_specs=VMEM,
        compiler_params=pltpu.CompilerParams(vmem_limit_bytes=8 * MIB),
        cost_estimate=pl.CostEstimate(
            flops=4 * tokens * width, bytes_accessed=18 * tokens * width, transcendentals=0
        ),
    )(at_home, from_before, from_after, from_two_before, from_two_after)
    return grad_weight, grad_context


def solution(mesh):
    return jax.shard_map(
        step,
        mesh=mesh,
        in_specs=(P(("batch", "seq"), "mp"), P(("batch", "seq"), "mp"), P(None, "mp")),
        out_specs=(P(("batch", "seq"), "mp"), P(("batch", "seq"), "mp")),
        check_vma=False,
    )
```

```python
import functools

import jax
import jax.numpy as jnp
from jax import lax
from jax.experimental import pallas as pl
from jax.experimental.pallas import tpu as pltpu
from jax.sharding import PartitionSpec as P


AXES = ("batch", "seq", "mp")
F32 = jnp.float32
BF16 = jnp.bfloat16
VMEM = pl.BlockSpec(memory_space=pltpu.VMEM)

MIB = 1 << 20


def here():
    batch, mp = lax.axis_index("batch"), lax.axis_index("mp")
    return batch & 1, mp >> 1, mp & 1


def place(x, h, y, l, c):
    return ((x * 2 + h) * 4 + y) * 8 + l * 2 + c


def pairs(route):
    return [
        (place(x, h, y, l, c), place(*route(x, h, y, l, c)))
        for x in range(4)
        for h in range(2)
        for y in range(4)
        for l in range(4)
        for c in range(2)
    ]


def ring(step):
    def route(x, h, y, l, c):
        z = (4 * h + l + step) % 8
        return x, z // 4, y, z % 4, c

    return route


def crosswise(k, first):
    def route(x, h, y, l, c):
        if (c == 0) == first:
            return x ^ k, h, y, l, c
        return x, h, y ^ k, l, c

    return route


def send(array, route):
    return lax.ppermute(array, AXES, pairs(route))


def products_kernel(kept, weight, near, far, *refs):
    h, l, c = here()
    turned = refs[-1]
    turned[0] = near[...].T
    turned[1] = far[...].T
    depth = near.shape[1]
    rows = depth // 2
    core = c if kept else 1 - c
    for i, (block, steps) in enumerate(((0, (0, 0)), (1, (1, 1)), (3, (-1, -1)), (2, (2, -2)))):
        for half, step in enumerate(steps):
            target = (4 * h + l + step + 8) & 7
            use_far = (target >> 2) ^ h
            row = ((((l + block) & 3) * 2 + core) * 2 + half) * rows
            part = pl.ds(half * rows, rows)
            total = jnp.dot(
                weight[pl.ds(pl.multiple_of(row, rows), rows), :],
                turned[use_far],
                preferred_element_type=F32,
            )
            if not kept:
                refs[0][i, part, :] = total
                continue
            total += refs[0][i, part, :]
            if i < 3:
                refs[1 + i][part, :] = total
            else:
                refs[4 + half][...] = total


def products(weight, near, far, *taken):
    tokens, depth = near.shape
    kept = bool(taken)
    if kept:
        rows = [depth, depth, depth, depth // 2, depth // 2]
        shapes = [jax.ShapeDtypeStruct((n, tokens), F32) for n in rows]
    else:
        shapes = [jax.ShapeDtypeStruct((4, depth, tokens), F32)]
    return pl.pallas_call(
        functools.partial(products_kernel, kept),
        out_shape=shapes,
        in_specs=[VMEM] * (3 + kept),
        out_specs=[VMEM] * len(shapes),
        scratch_shapes=[pltpu.VMEM((2, depth, tokens), BF16)],
        compiler_params=pltpu.CompilerParams(vmem_limit_bytes=20 * MIB),
        cost_estimate=pl.CostEstimate(
            flops=8 * depth * tokens * depth,
            bytes_accessed=8 * depth * depth + 16 * depth * tokens,
            transcendentals=0,
        ),
    )(weight, near, far, *taken)


def pair_kernel(near, far, out):
    tokens = near.shape[0]
    out[pl.ds(0, tokens), :] = near[...]
    out[pl.ds(tokens, tokens), :] = far[...]


def finish_kernel(home, before, after, two_before, two_after, out):
    rows = two_before.shape[0]
    for i, skip in enumerate((two_before, two_after)):
        part = pl.ds(i * rows, rows)
        total = home[part, :] + before[part, :] + after[part, :] + skip[...]
        out[:, part] = total.T.astype(BF16)


def weight_kernel(items, own, other, *refs):
    h, low, core = here()
    swapped = core != h
    y = lax.axis_index("seq")
    arrays = 1 + max(max(item[0], item[2]) for item in items)
    tokens = own.shape[3]
    out = refs[-1]
    total = refs[arrays][...] if len(refs) > arrays + 1 else jnp.zeros(out.shape, F32)
    for a, row, b, far_row, i, j in items:
        k = low ^ jnp.where(core == 0, i, j)
        s = y ^ jnp.where(core == 0, j, i)
        mine, theirs = own[k, s], other[k, s]
        near = jnp.where(swapped, theirs, mine)
        far = jnp.where(swapped, mine, theirs)
        left = jnp.concatenate([near, far], axis=1)
        right = jnp.concatenate(
            [refs[a][pl.ds(row, tokens), :], refs[b][pl.ds(far_row, tokens), :]]
        )
        total += jnp.dot(left, right, preferred_element_type=F32)
    out[...] = total


def weight_part(items, own, other, arrays, *total):
    rows, width = own.shape[2], arrays[0].shape[1]
    depth = 2 * own.shape[3] * len(items)
    return pl.pallas_call(
        functools.partial(weight_kernel, items),
        out_shape=jax.ShapeDtypeStruct((rows, width), F32),
        in_specs=[VMEM] * (2 + len(arrays) + len(total)),
        out_specs=VMEM,
        compiler_params=pltpu.CompilerParams(vmem_limit_bytes=16 * MIB),
        cost_estimate=pl.CostEstimate(
            flops=2 * rows * width * depth,
            bytes_accessed=2 * depth * (width + rows) + 8 * rows * width,
            transcendentals=0,
        ),
    )(own, other, *arrays, *total)


def step(context, cotangent, out_weight):
    tokens, width = cotangent.shape
    quarter = width // 4

    others = (1, 2, 3)

    far_cot = send(cotangent, ring(4))
    pair = pl.pallas_call(
        pair_kernel,
        out_shape=jax.ShapeDtypeStruct((2 * tokens, width), BF16),
        in_specs=[VMEM] * 2,
        out_specs=VMEM,
        compiler_params=pltpu.CompilerParams(vmem_limit_bytes=4 * MIB),
        cost_estimate=pl.CostEstimate(
            flops=0, bytes_accessed=8 * tokens * width, transcendentals=0
        ),
    )(cotangent, far_cot)
    first = [send(pair, crosswise(k, True)) for k in others]
    second = [send(cotangent, crosswise(k, False)) for k in others]
    row = jnp.concatenate([*first, far_cot])
    one, three = (send(row, crosswise(k, False)) for k in (1, 3))
    cut = 4 * tokens
    two = [send(three[:cut], crosswise(1, False)), send(one[cut:], crosswise(3, False))]

    turned = context.T.reshape(4, quarter, tokens)
    block = lax.all_to_all(turned, "seq", split_axis=0, concat_axis=0, tiled=True)
    mine = send(block, lambda x, h, y, l, c: (l, c, y, l ^ x, h))
    gathered = [mine] + [
        send(mine, lambda x, h, y, l, c, k=k: (x, h, y, l ^ k, c)) for k in (1, 2, 3)
    ]
    own = jnp.stack(gathered)
    swap = lambda x, h, y, l, c: (x, h, y, l, 1 - c)
    other = send(own, swap)

    (given,) = products(out_weight, cotangent, far_cot)
    taken = send(given, swap)
    at_home, after, before, skip_up, skip_down = products(out_weight, cotangent, far_cot, taken)
    from_before = send(after, ring(1))
    from_after = send(before, ring(-1))
    from_two_before = send(skip_up, ring(2))
    from_two_after = send(skip_down, ring(-2))

    early = [(k, 0, k, tokens, k, 0) for k in range(4)]
    both = [one, three, second[0], second[2]]
    late = [
        (2 + a, 0, a, 6 * tokens, 0, k) if i == 0 else (a, at_row, a, at_row + tokens, i, k)
        for a, k in ((0, 1), (1, 3))
        for i in range(4)
        for at_row in (2 * tokens * (i - 1),)
    ]
    last = [
        (0, 0, 0, tokens, 1, 2),
        (0, 2 * tokens, 0, 3 * tokens, 2, 2),
        (1, 0, 1, tokens, 3, 2),
        (2, 0, 1, 2 * tokens, 0, 2),
    ]
    total = weight_part(early, own, other, [pair] + first)
    total = weight_part(late, own, other, both, total)
    grad_weight = weight_part(last, own, other, two + [second[1]], total)
    grad_context = pl.pallas_call(
        finish_kernel,
        out_shape=jax.ShapeDtypeStruct((tokens, width), BF16),
        in_specs=[VMEM] * 5,
        out_specs=VMEM,
        compiler_params=pltpu.CompilerParams(vmem_limit_bytes=8 * MIB),
        cost_estimate=pl.CostEstimate(
            flops=4 * tokens * width, bytes_accessed=18 * tokens * width, transcendentals=0
        ),
    )(at_home, from_before, from_after, from_two_before, from_two_after)
    return grad_weight, grad_context


def solution(mesh):
    return jax.shard_map(
        step,
        mesh=mesh,
        in_specs=(P(("batch", "seq"), "mp"), P(("batch", "seq"), "mp"), P(None, "mp")),
        out_specs=(P(("batch", "seq"), "mp"), P(("batch", "seq"), "mp")),
        check_vma=False,
    )
```

```python
import functools

import jax
import jax.numpy as jnp
from jax import lax
from jax.experimental import pallas as pl
from jax.experimental.pallas import tpu as pltpu
from jax.sharding import PartitionSpec as P


AXES = ("batch", "seq", "mp")
F32 = jnp.float32
BF16 = jnp.bfloat16
VMEM = pl.BlockSpec(memory_space=pltpu.VMEM)

MIB = 1 << 20


def here():
    batch, mp = lax.axis_index("batch"), lax.axis_index("mp")
    return batch & 1, mp >> 1, mp & 1


def place(x, h, y, l, c):
    return ((x * 2 + h) * 4 + y) * 8 + l * 2 + c


def pairs(route):
    return [
        (place(x, h, y, l, c), place(*route(x, h, y, l, c)))
        for x in range(4)
        for h in range(2)
        for y in range(4)
        for l in range(4)
        for c in range(2)
    ]


def ring(step):
    def route(x, h, y, l, c):
        z = (4 * h + l + step) % 8
        return x, z // 4, y, z % 4, c

    return route


def crosswise(k, first):
    def route(x, h, y, l, c):
        if (c == 0) == first:
            return x ^ k, h, y, l, c
        return x, h, y ^ k, l, c

    return route


def send(array, route):
    return lax.ppermute(array, AXES, pairs(route))


def at(stack, index):
    return lax.dynamic_index_in_dim(stack, index, 0, keepdims=False)


def products_kernel(kept, weight, near, far, *refs):
    h, l, c = here()
    turned = refs[-1]
    turned[0] = near[...].T
    turned[1] = far[...].T
    depth = near.shape[1]
    rows = depth // 2
    core = c if kept else 1 - c
    for i, (block, steps) in enumerate(((0, (0, 0)), (1, (1, 1)), (3, (-1, -1)), (2, (2, -2)))):
        for half, step in enumerate(steps):
            target = (4 * h + l + step + 8) & 7
            use_far = (target >> 2) ^ h
            row = ((((l + block) & 3) * 2 + core) * 2 + half) * rows
            part = pl.ds(half * rows, rows)
            total = jnp.dot(
                weight[pl.ds(pl.multiple_of(row, rows), rows), :],
                turned[use_far],
                preferred_element_type=F32,
            )
            if not kept:
                refs[0][i, part, :] = total
                continue
            total += refs[0][i, part, :]
            if i < 3:
                refs[1 + i][part, :] = total
            else:
                refs[4 + half][...] = total


def products(weight, near, far, *taken):
    tokens, depth = near.shape
    kept = bool(taken)
    if kept:
        rows = [depth, depth, depth, depth // 2, depth // 2]
        shapes = [jax.ShapeDtypeStruct((n, tokens), F32) for n in rows]
    else:
        shapes = [jax.ShapeDtypeStruct((4, depth, tokens), F32)]
    return pl.pallas_call(
        functools.partial(products_kernel, kept),
        out_shape=shapes,
        in_specs=[VMEM] * (3 + kept),
        out_specs=[VMEM] * len(shapes),
        scratch_shapes=[pltpu.VMEM((2, depth, tokens), BF16)],
        compiler_params=pltpu.CompilerParams(vmem_limit_bytes=20 * MIB),
        cost_estimate=pl.CostEstimate(
            flops=8 * depth * tokens * depth,
            bytes_accessed=8 * depth * depth + 16 * depth * tokens,
            transcendentals=0,
        ),
    )(weight, near, far, *taken)


def finish_kernel(home, before, after, two_before, two_after, out):
    rows = two_before.shape[0]
    for i, skip in enumerate((two_before, two_after)):
        part = pl.ds(i * rows, rows)
        total = home[part, :] + before[part, :] + after[part, :] + skip[...]
        out[:, part] = total.T.astype(BF16)


def weight_kernel(items, own, other, *refs):
    h, low, core = here()
    swapped = core != h
    arrays = 1 + max(max(item[0], item[2]) for item in items)
    tokens = own.shape[3]
    out = refs[-1]
    total = refs[arrays][...] if len(refs) > arrays + 1 else jnp.zeros(out.shape, F32)
    for a, row, b, far_row, i, j in items:
        k = low ^ jnp.where(core == 0, i, j)
        s = jnp.where(core == 0, j, i)
        mine, theirs = own[k, s], other[k, s]
        near = jnp.where(swapped, theirs, mine)
        far = jnp.where(swapped, mine, theirs)
        left = jnp.concatenate([near, far], axis=1)
        right = jnp.concatenate(
            [refs[a][pl.ds(row, tokens), :], refs[b][pl.ds(far_row, tokens), :]]
        )
        total += jnp.dot(left, right, preferred_element_type=F32)
    out[...] = total


def weight_part(items, own, other, arrays, *total):
    rows, width = own.shape[2], arrays[0].shape[1]
    depth = 2 * own.shape[3] * len(items)
    return pl.pallas_call(
        functools.partial(weight_kernel, items),
        out_shape=jax.ShapeDtypeStruct((rows, width), F32),
        in_specs=[VMEM] * (2 + len(arrays) + len(total)),
        out_specs=VMEM,
        compiler_params=pltpu.CompilerParams(vmem_limit_bytes=16 * MIB),
        cost_estimate=pl.CostEstimate(
            flops=2 * rows * width * depth,
            bytes_accessed=2 * depth * (width + rows) + 8 * rows * width,
            transcendentals=0,
        ),
    )(own, other, *arrays, *total)


def step(context, cotangent, out_weight):
    y = lax.axis_index("seq")
    tokens, width = cotangent.shape
    quarter = width // 4

    others = (1, 2, 3)

    far_cot = send(cotangent, ring(4))
    pair = jnp.concatenate([cotangent, far_cot])
    first = [send(pair, crosswise(k, True)) for k in others]
    row = jnp.concatenate([*first, pair])
    one, three = (send(row, crosswise(k, False)) for k in (1, 3))
    cut = 4 * tokens
    two = [send(three[:cut], crosswise(1, False)), send(one[cut:], crosswise(3, False))]

    turned = context.T.reshape(4, quarter, tokens)
    block = jnp.stack(
        [at(turned, y)]
        + [send(at(turned, y ^ k), lambda x, h, y, l, c, k=k: (x, h, y ^ k, l, c)) for k in others]
    )
    mine = send(block, lambda x, h, y, l, c: (l, c, y, l ^ x, h))
    gathered = [mine] + [
        send(mine, lambda x, h, y, l, c, k=k: (x, h, y, l ^ k, c)) for k in (1, 2, 3)
    ]
    own = jnp.stack(gathered)
    swap = lambda x, h, y, l, c: (x, h, y, l, 1 - c)
    other = send(own, swap)

    (given,) = products(out_weight, cotangent, far_cot)
    taken = send(given, swap)
    at_home, after, before, skip_up, skip_down = products(out_weight, cotangent, far_cot, taken)
    from_before = send(after, ring(1))
    from_after = send(before, ring(-1))
    from_two_before = send(skip_up, ring(2))
    from_two_after = send(skip_down, ring(-2))

    early = [(k, 0, k, tokens, k, 0) for k in range(4)]
    late = [
        (a, at_row, a, at_row + tokens, i, k)
        for a, k in ((0, 1), (1, 3))
        for i in range(4)
        for at_row in (2 * tokens * ((i + 3) % 4),)
    ]
    last = [
        (a, at_row, a, at_row + tokens, i, 2)
        for a, at_row, i in ((0, 0, 1), (0, 2 * tokens, 2), (1, 0, 3), (1, 2 * tokens, 0))
    ]
    total = weight_part(early, own, other, [pair] + first)
    total = weight_part(late, own, other, [one, three], total)
    grad_weight = weight_part(last, own, other, two, total)
    grad_context = pl.pallas_call(
        finish_kernel,
        out_shape=jax.ShapeDtypeStruct((tokens, width), BF16),
        in_specs=[VMEM] * 5,
        out_specs=VMEM,
        compiler_params=pltpu.CompilerParams(vmem_limit_bytes=8 * MIB),
        cost_estimate=pl.CostEstimate(
            flops=4 * tokens * width, bytes_accessed=18 * tokens * width, transcendentals=0
        ),
    )(at_home, from_before, from_after, from_two_before, from_two_after)
    return grad_weight, grad_context


def solution(mesh):
    return jax.shard_map(
        step,
        mesh=mesh,
        in_specs=(P(("batch", "seq"), "mp"), P(("batch", "seq"), "mp"), P(None, "mp")),
        out_specs=(P(("batch", "seq"), "mp"), P(("batch", "seq"), "mp")),
        check_vma=False,
    )
```

```python
import functools

import jax
import jax.numpy as jnp
from jax import lax
from jax.experimental import pallas as pl
from jax.experimental.pallas import tpu as pltpu
from jax.sharding import PartitionSpec as P


AXES = ("batch", "seq", "mp")
F32 = jnp.float32
BF16 = jnp.bfloat16
VMEM = pl.BlockSpec(memory_space=pltpu.VMEM)

MIB = 1 << 20


def here():
    batch, mp = lax.axis_index("batch"), lax.axis_index("mp")
    return batch & 1, mp >> 1, mp & 1


def place(x, h, y, l, c):
    return ((x * 2 + h) * 4 + y) * 8 + l * 2 + c


def pairs(route):
    return [
        (place(x, h, y, l, c), place(*route(x, h, y, l, c)))
        for x in range(4)
        for h in range(2)
        for y in range(4)
        for l in range(4)
        for c in range(2)
    ]


def ring(step):
    def route(x, h, y, l, c):
        z = (4 * h + l + step) % 8
        return x, z // 4, y, z % 4, c

    return route


def crosswise(k, first):
    def route(x, h, y, l, c):
        if (c == 0) == first:
            return x ^ k, h, y, l, c
        return x, h, y ^ k, l, c

    return route


def send(array, route):
    return lax.ppermute(array, AXES, pairs(route))


def at(stack, index):
    return lax.dynamic_index_in_dim(stack, index, 0, keepdims=False)


def products_kernel(kept, weight, near, far, *refs):
    h, l, c = here()
    turned = refs[-1]
    if not kept:
        refs = refs[1:]
    turned[0] = near[...].T
    turned[1] = far[...].T
    depth = near.shape[1]
    rows = depth // 2
    core = c if kept else 1 - c
    for i, (block, steps) in enumerate(((0, (0, 0)), (1, (1, 1)), (3, (-1, -1)), (2, (2, -2)))):
        for half, step in enumerate(steps):
            target = (4 * h + l + step + 8) & 7
            use_far = (target >> 2) ^ h
            row = ((((l + block) & 3) * 2 + core) * 2 + half) * rows
            part = pl.ds(half * rows, rows)
            total = jnp.dot(
                weight[pl.ds(pl.multiple_of(row, rows), rows), :],
                turned[use_far],
                preferred_element_type=F32,
            )
            if not kept:
                refs[0][i, part, :] = total
                continue
            total += refs[0][i, part, :]
            if i < 3:
                refs[1 + i][part, :] = total
            else:
                refs[4 + half][...] = total


def products(weight, near, far, *taken, after=None):
    tokens, depth = near.shape
    kept = bool(taken)
    if after is not None:
        taken = (after,)
    if kept:
        rows = [depth, depth, depth, depth // 2, depth // 2]
        shapes = [jax.ShapeDtypeStruct((n, tokens), F32) for n in rows]
    else:
        shapes = [jax.ShapeDtypeStruct((4, depth, tokens), F32)]
    return pl.pallas_call(
        functools.partial(products_kernel, kept),
        out_shape=shapes,
        in_specs=[VMEM] * (3 + len(taken)),
        out_specs=[VMEM] * len(shapes),
        scratch_shapes=[pltpu.VMEM((2, depth, tokens), BF16)],
        compiler_params=pltpu.CompilerParams(vmem_limit_bytes=20 * MIB),
        cost_estimate=pl.CostEstimate(
            flops=8 * depth * tokens * depth,
            bytes_accessed=8 * depth * depth + 16 * depth * tokens,
            transcendentals=0,
        ),
    )(weight, near, far, *taken)


def touch_kernel(weight, out):
    out[...] = weight[pl.ds(0, 16), pl.ds(0, 128)]


def finish_kernel(home, before, after, two_before, two_after, out):
    rows = two_before.shape[0]
    for i, skip in enumerate((two_before, two_after)):
        part = pl.ds(i * rows, rows)
        total = home[part, :] + before[part, :] + after[part, :] + skip[...]
        out[:, part] = total.T.astype(BF16)


def weight_kernel(items, own, other, *refs):
    h, low, core = here()
    swapped = core != h
    arrays = 1 + max(max(item[0], item[2]) for item in items)
    tokens = own.shape[3]
    out = refs[-1]
    total = refs[arrays][...] if len(refs) > arrays + 1 else jnp.zeros(out.shape, F32)
    for a, row, b, far_row, i, j in items:
        k = low ^ jnp.where(core == 0, i, j)
        s = jnp.where(core == 0, j, i)
        mine, theirs = own[k, s], other[k, s]
        near = jnp.where(swapped, theirs, mine)
        far = jnp.where(swapped, mine, theirs)
        left = jnp.concatenate([near, far], axis=1)
        right = jnp.concatenate(
            [refs[a][pl.ds(row, tokens), :], refs[b][pl.ds(far_row, tokens), :]]
        )
        total += jnp.dot(left, right, preferred_element_type=F32)
    out[...] = total


def weight_part(items, own, other, arrays, *total):
    rows, width = own.shape[2], arrays[0].shape[1]
    depth = 2 * own.shape[3] * len(items)
    return pl.pallas_call(
        functools.partial(weight_kernel, items),
        out_shape=jax.ShapeDtypeStruct((rows, width), F32),
        in_specs=[VMEM] * (2 + len(arrays) + len(total)),
        out_specs=VMEM,
        compiler_params=pltpu.CompilerParams(vmem_limit_bytes=16 * MIB),
        cost_estimate=pl.CostEstimate(
            flops=2 * rows * width * depth,
            bytes_accessed=2 * depth * (width + rows) + 8 * rows * width,
            transcendentals=0,
        ),
    )(own, other, *arrays, *total)


def step(context, cotangent, out_weight):
    y = lax.axis_index("seq")
    tokens, width = cotangent.shape
    quarter = width // 4

    others = (1, 2, 3)

    far_cot = send(cotangent, ring(4))
    pair = jnp.concatenate([cotangent, far_cot])
    first = [send(pair, crosswise(k, True)) for k in others]
    low_half = jnp.concatenate(first[:2])
    high_half = jnp.concatenate([first[2], pair])
    low3 = send(low_half, crosswise(3, False))
    high1 = send(high_half, crosswise(1, False))
    high3 = send(high_half, crosswise(3, False))
    low1 = send(low_half, crosswise(1, False))
    low2 = send(low3, crosswise(1, False))
    high2 = send(high1, crosswise(3, False))

    turned = context.T.reshape(4, quarter, tokens)
    block = jnp.stack(
        [at(turned, y)]
        + [send(at(turned, y ^ k), lambda x, h, y, l, c, k=k: (x, h, y ^ k, l, c)) for k in others]
    )
    mine = send(block, lambda x, h, y, l, c: (l, c, y, l ^ x, h))
    gathered = [mine] + [
        send(mine, lambda x, h, y, l, c, k=k: (x, h, y, l ^ k, c)) for k in (1, 2, 3)
    ]
    own = jnp.stack(gathered)
    swap = lambda x, h, y, l, c: (x, h, y, l, 1 - c)
    other = send(own, swap)

    corner = pl.pallas_call(
        touch_kernel,
        out_shape=jax.ShapeDtypeStruct((16, 128), BF16),
        in_specs=[VMEM],
        out_specs=VMEM,
        compiler_params=pltpu.CompilerParams(vmem_limit_bytes=12 * MIB),
        cost_estimate=pl.CostEstimate(flops=0, bytes_accessed=8192, transcendentals=0),
    )(out_weight)
    (given,) = products(out_weight, cotangent, far_cot, after=corner)
    taken = send(given, swap)
    at_home, after, before, skip_up, skip_down = products(out_weight, cotangent, far_cot, taken)
    from_before = send(after, ring(1))
    from_after = send(before, ring(-1))
    from_two_before = send(skip_up, ring(2))
    from_two_after = send(skip_down, ring(-2))

    early = [(k, 0, k, tokens, k, 0) for k in range(4)]
    halves = lambda a, k: [
        (a + n // 2, deep, a + n // 2, deep + tokens, i, k)
        for n, i in enumerate((1, 2, 3, 0))
        for deep in (n % 2 * 2 * tokens,)
    ]
    total = weight_part(early, own, other, [pair] + first)
    total = weight_part(halves(0, 1) + halves(2, 3), own, other, [low1, high1, low3, high3], total)
    grad_weight = weight_part(halves(0, 2), own, other, [low2, high2], total)
    grad_context = pl.pallas_call(
        finish_kernel,
        out_shape=jax.ShapeDtypeStruct((tokens, width), BF16),
        in_specs=[VMEM] * 5,
        out_specs=VMEM,
        compiler_params=pltpu.CompilerParams(vmem_limit_bytes=8 * MIB),
        cost_estimate=pl.CostEstimate(
            flops=4 * tokens * width, bytes_accessed=18 * tokens * width, transcendentals=0
        ),
    )(at_home, from_before, from_after, from_two_before, from_two_after)
    return grad_weight, grad_context


def solution(mesh):
    return jax.shard_map(
        step,
        mesh=mesh,
        in_specs=(P(("batch", "seq"), "mp"), P(("batch", "seq"), "mp"), P(None, "mp")),
        out_specs=(P(("batch", "seq"), "mp"), P(("batch", "seq"), "mp")),
        check_vma=False,
    )
```

```python
import functools

import jax
import jax.numpy as jnp
from jax import lax
from jax.experimental import pallas as pl
from jax.experimental.pallas import tpu as pltpu
from jax.sharding import PartitionSpec as P


AXES = ("batch", "seq", "mp")
F32 = jnp.float32
BF16 = jnp.bfloat16
VMEM = pl.BlockSpec(memory_space=pltpu.VMEM)

MIB = 1 << 20


def here():
    batch, mp = lax.axis_index("batch"), lax.axis_index("mp")
    return batch & 1, mp >> 1, mp & 1


def place(x, h, y, l, c):
    return ((x * 2 + h) * 4 + y) * 8 + l * 2 + c


def pairs(route):
    return [
        (place(x, h, y, l, c), place(*route(x, h, y, l, c)))
        for x in range(4)
        for h in range(2)
        for y in range(4)
        for l in range(4)
        for c in range(2)
    ]


def ring(step):
    def route(x, h, y, l, c):
        z = (4 * h + l + step) % 8
        return x, z // 4, y, z % 4, c

    return route


def crosswise(k, first):
    def route(x, h, y, l, c):
        if (c == 0) == first:
            return x ^ k, h, y, l, c
        return x, h, y ^ k, l, c

    return route


def send(array, route):
    return lax.ppermute(array, AXES, pairs(route))


def at(stack, index):
    return lax.dynamic_index_in_dim(stack, index, 0, keepdims=False)


def products_kernel(kept, weight, near, far, *refs):
    h, l, c = here()
    turned = refs[-1]
    if not kept:
        refs = refs[1:]
    turned[0] = near[...].T
    turned[1] = far[...].T
    depth = near.shape[1]
    rows = depth // 2
    core = c if kept else 1 - c
    for i, (block, steps) in enumerate(((0, (0, 0)), (1, (1, 1)), (3, (-1, -1)), (2, (2, -2)))):
        for half, step in enumerate(steps):
            target = (4 * h + l + step + 8) & 7
            use_far = (target >> 2) ^ h
            row = ((((l + block) & 3) * 2 + core) * 2 + half) * rows
            part = pl.ds(half * rows, rows)
            total = jnp.dot(
                weight[pl.ds(pl.multiple_of(row, rows), rows), :],
                turned[use_far],
                preferred_element_type=F32,
            )
            if not kept:
                refs[0][i, part, :] = total
                continue
            total += refs[0][i, part, :]
            if i < 3:
                refs[1 + i][part, :] = total
            else:
                refs[4 + half][...] = total


def products(weight, near, far, *taken, after=None):
    tokens, depth = near.shape
    kept = bool(taken)
    if after is not None:
        taken = (after,)
    if kept:
        rows = [depth, depth, depth, depth // 2, depth // 2]
        shapes = [jax.ShapeDtypeStruct((n, tokens), F32) for n in rows]
    else:
        shapes = [jax.ShapeDtypeStruct((4, depth, tokens), F32)]
    return pl.pallas_call(
        functools.partial(products_kernel, kept),
        out_shape=shapes,
        in_specs=[VMEM] * (3 + len(taken)),
        out_specs=[VMEM] * len(shapes),
        scratch_shapes=[pltpu.VMEM((2, depth, tokens), BF16)],
        compiler_params=pltpu.CompilerParams(vmem_limit_bytes=20 * MIB),
        cost_estimate=pl.CostEstimate(
            flops=8 * depth * tokens * depth,
            bytes_accessed=8 * depth * depth + 16 * depth * tokens,
            transcendentals=0,
        ),
    )(weight, near, far, *taken)


def touch_kernel(weight, out):
    out[...] = weight[pl.ds(0, 16), pl.ds(0, 128)]


def finish_kernel(home, before, after, two_before, two_after, out):
    rows = two_before.shape[0]
    for i, skip in enumerate((two_before, two_after)):
        part = pl.ds(i * rows, rows)
        total = home[part, :] + before[part, :] + after[part, :] + skip[...]
        out[:, part] = total.T.astype(BF16)


def weight_kernel(items, own, other, *refs):
    h, low, core = here()
    swapped = core != h
    arrays = 1 + max(max(item[0], item[2]) for item in items)
    tokens = own.shape[3]
    out = refs[-1]
    total = refs[arrays][...] if len(refs) > arrays + 1 else jnp.zeros(out.shape, F32)
    for a, row, b, far_row, i, j in items:
        k = low ^ jnp.where(core == 0, i, j)
        s = jnp.where(core == 0, j, i)
        mine, theirs = own[k, s], other[k, s]
        near = jnp.where(swapped, theirs, mine)
        far = jnp.where(swapped, mine, theirs)
        left = jnp.concatenate([near, far], axis=1)
        right = jnp.concatenate(
            [refs[a][pl.ds(row, tokens), :], refs[b][pl.ds(far_row, tokens), :]]
        )
        total += jnp.dot(left, right, preferred_element_type=F32)
    out[...] = total


def weight_part(items, own, other, arrays, *total):
    rows, width = own.shape[2], arrays[0].shape[1]
    depth = 2 * own.shape[3] * len(items)
    return pl.pallas_call(
        functools.partial(weight_kernel, items),
        out_shape=jax.ShapeDtypeStruct((rows, width), F32),
        in_specs=[VMEM] * (2 + len(arrays) + len(total)),
        out_specs=VMEM,
        compiler_params=pltpu.CompilerParams(vmem_limit_bytes=16 * MIB),
        cost_estimate=pl.CostEstimate(
            flops=2 * rows * width * depth,
            bytes_accessed=2 * depth * (width + rows) + 8 * rows * width,
            transcendentals=0,
        ),
    )(own, other, *arrays, *total)


def step(context, cotangent, out_weight):
    y = lax.axis_index("seq")
    tokens, width = cotangent.shape
    quarter = width // 4

    others = (1, 2, 3)

    far_cot = send(cotangent, ring(4))
    pair = jnp.concatenate([cotangent, far_cot])
    first = [send(pair, crosswise(k, True)) for k in others]
    half_a = jnp.concatenate([pair, first[0]])
    half_b = jnp.concatenate([first[2], first[1]])
    a1 = send(half_a, crosswise(1, False))
    a3 = send(half_a, crosswise(3, False))
    b3 = send(half_b, crosswise(3, False))
    b1 = send(half_b, crosswise(1, False))
    a2 = send(a3, crosswise(1, False))
    b2 = send(b1, crosswise(3, False))

    turned = context.T.reshape(4, quarter, tokens)
    block = jnp.stack(
        [at(turned, y)]
        + [send(at(turned, y ^ k), lambda x, h, y, l, c, k=k: (x, h, y ^ k, l, c)) for k in others]
    )
    mine = send(block, lambda x, h, y, l, c: (l, c, y, l ^ x, h))
    along = lambda k: lambda x, h, y, l, c: (x, h, y, l ^ k, c)
    three_away = send(mine, along(3))
    next_one = send(mine, along(1))
    gathered = [mine, next_one, send(three_away, along(1)), three_away]
    own = jnp.stack(gathered)
    swap = lambda x, h, y, l, c: (x, h, y, l, 1 - c)
    other = send(own, swap)

    corner = pl.pallas_call(
        touch_kernel,
        out_shape=jax.ShapeDtypeStruct((16, 128), BF16),
        in_specs=[VMEM],
        out_specs=VMEM,
        compiler_params=pltpu.CompilerParams(vmem_limit_bytes=12 * MIB),
        cost_estimate=pl.CostEstimate(flops=0, bytes_accessed=8192, transcendentals=0),
    )(out_weight)
    (given,) = products(out_weight, cotangent, far_cot, after=corner)
    taken = send(given, swap)
    at_home, after, before, skip_up, skip_down = products(out_weight, cotangent, far_cot, taken)
    from_before = send(after, ring(1))
    from_after = send(before, ring(-1))
    from_two_before = send(skip_up, ring(2))
    from_two_after = send(skip_down, ring(-2))

    early = [(k, 0, k, tokens, k, 0) for k in range(4)]
    halves = lambda a, k: [
        (a + n // 2, deep, a + n // 2, deep + tokens, i, k)
        for n, i in enumerate((0, 1, 3, 2))
        for deep in (n % 2 * 2 * tokens,)
    ]
    total = weight_part(early, own, other, [pair] + first)
    total = weight_part(halves(0, 1) + halves(2, 3), own, other, [a1, b1, a3, b3], total)
    grad_weight = weight_part(halves(0, 2), own, other, [a2, b2], total)
    grad_context = pl.pallas_call(
        finish_kernel,
        out_shape=jax.ShapeDtypeStruct((tokens, width), BF16),
        in_specs=[VMEM] * 5,
        out_specs=VMEM,
        compiler_params=pltpu.CompilerParams(vmem_limit_bytes=8 * MIB),
        cost_estimate=pl.CostEstimate(
            flops=4 * tokens * width, bytes_accessed=18 * tokens * width, transcendentals=0
        ),
    )(at_home, from_before, from_after, from_two_before, from_two_after)
    return grad_weight, grad_context


def solution(mesh):
    return jax.shard_map(
        step,
        mesh=mesh,
        in_specs=(P(("batch", "seq"), "mp"), P(("batch", "seq"), "mp"), P(None, "mp")),
        out_specs=(P(("batch", "seq"), "mp"), P(("batch", "seq"), "mp")),
        check_vma=False,
    )
```

```python
import functools

import jax
import jax.numpy as jnp
from jax import lax
from jax.experimental import pallas as pl
from jax.experimental.pallas import tpu as pltpu
from jax.sharding import PartitionSpec as P


AXES = ("batch", "seq", "mp")
F32 = jnp.float32
BF16 = jnp.bfloat16
VMEM = pl.BlockSpec(memory_space=pltpu.VMEM)

MIB = 1 << 20


def here():
    batch, mp = lax.axis_index("batch"), lax.axis_index("mp")
    return batch & 1, mp >> 1, mp & 1


def place(x, h, y, l, c):
    return ((x * 2 + h) * 4 + y) * 8 + l * 2 + c


def pairs(route):
    return [
        (place(x, h, y, l, c), place(*route(x, h, y, l, c)))
        for x in range(4)
        for h in range(2)
        for y in range(4)
        for l in range(4)
        for c in range(2)
    ]


def ring(step):
    def route(x, h, y, l, c):
        z = (4 * h + l + step) % 8
        return x, z // 4, y, z % 4, c

    return route


def crosswise(k, first):
    def route(x, h, y, l, c):
        if (c == 0) == first:
            return x ^ k, h, y, l, c
        return x, h, y ^ k, l, c

    return route


def send(array, route):
    return lax.ppermute(array, AXES, pairs(route))


def at(stack, index):
    return lax.dynamic_index_in_dim(stack, index, 0, keepdims=False)


def products_kernel(kept, weight, near, far, *refs):
    h, l, c = here()
    turned = refs[-1]
    if not kept:
        refs = refs[1:]
    turned[0] = near[...].T
    turned[1] = far[...].T
    depth = near.shape[1]
    rows = depth // 2
    core = c if kept else 1 - c
    for i, (block, steps) in enumerate(((0, (0, 0)), (1, (1, 1)), (3, (-1, -1)), (2, (2, -2)))):
        for half, step in enumerate(steps):
            target = (4 * h + l + step + 8) & 7
            use_far = (target >> 2) ^ h
            row = ((((l + block) & 3) * 2 + core) * 2 + half) * rows
            part = pl.ds(half * rows, rows)
            total = jnp.dot(
                weight[pl.ds(pl.multiple_of(row, rows), rows), :],
                turned[use_far],
                preferred_element_type=F32,
            )
            if not kept:
                refs[0][i, part, :] = total
                continue
            total += refs[0][i, part, :]
            if i < 3:
                refs[1 + i][part, :] = total
            else:
                refs[4 + half][...] = total


def products(weight, near, far, *taken, after=None):
    tokens, depth = near.shape
    kept = bool(taken)
    if after is not None:
        taken = (after,)
    if kept:
        rows = [depth, depth, depth, depth // 2, depth // 2]
        shapes = [jax.ShapeDtypeStruct((n, tokens), F32) for n in rows]
    else:
        shapes = [jax.ShapeDtypeStruct((4, depth, tokens), F32)]
    return pl.pallas_call(
        functools.partial(products_kernel, kept),
        out_shape=shapes,
        in_specs=[VMEM] * (3 + len(taken)),
        out_specs=[VMEM] * len(shapes),
        scratch_shapes=[pltpu.VMEM((2, depth, tokens), BF16)],
        compiler_params=pltpu.CompilerParams(vmem_limit_bytes=20 * MIB),
        cost_estimate=pl.CostEstimate(
            flops=8 * depth * tokens * depth,
            bytes_accessed=8 * depth * depth + 16 * depth * tokens,
            transcendentals=0,
        ),
    )(weight, near, far, *taken)


def touch_kernel(weight, out):
    out[...] = weight[pl.ds(0, 16), pl.ds(0, 128)]


def finish_kernel(home, before, after, two_before, two_after, out):
    rows = two_before.shape[0]
    for i, skip in enumerate((two_before, two_after)):
        part = pl.ds(i * rows, rows)
        total = home[part, :] + before[part, :] + after[part, :] + skip[...]
        out[:, part] = total.T.astype(BF16)


def weight_kernel(items, own, other, *refs):
    h, low, core = here()
    swapped = core != h
    arrays = 1 + max(max(item[0], item[2]) for item in items)
    tokens = own.shape[3]
    out = refs[-1]
    total = refs[arrays][...] if len(refs) > arrays + 1 else jnp.zeros(out.shape, F32)
    for a, row, b, far_row, i, j in items:
        k = low ^ jnp.where(core == 0, i, j)
        s = jnp.where(core == 0, j, i)
        mine, theirs = own[k, s], other[k, s]
        near = jnp.where(swapped, theirs, mine)
        far = jnp.where(swapped, mine, theirs)
        left = jnp.concatenate([near, far], axis=1)
        right = jnp.concatenate(
            [refs[a][pl.ds(row, tokens), :], refs[b][pl.ds(far_row, tokens), :]]
        )
        total += jnp.dot(left, right, preferred_element_type=F32)
    out[...] = total


def weight_part(items, own, other, arrays, *total):
    rows, width = own.shape[2], arrays[0].shape[1]
    depth = 2 * own.shape[3] * len(items)
    return pl.pallas_call(
        functools.partial(weight_kernel, items),
        out_shape=jax.ShapeDtypeStruct((rows, width), F32),
        in_specs=[VMEM] * (2 + len(arrays) + len(total)),
        out_specs=VMEM,
        compiler_params=pltpu.CompilerParams(vmem_limit_bytes=16 * MIB),
        cost_estimate=pl.CostEstimate(
            flops=2 * rows * width * depth,
            bytes_accessed=2 * depth * (width + rows) + 8 * rows * width,
            transcendentals=0,
        ),
    )(own, other, *arrays, *total)


def step(context, cotangent, out_weight):
    y = lax.axis_index("seq")
    tokens, width = cotangent.shape
    quarter = width // 4

    others = (1, 2, 3)

    far_cot = send(cotangent, ring(4))
    pair = jnp.concatenate([cotangent, far_cot])
    first = [send(pair, crosswise(k, True)) for k in others]
    half_a = jnp.concatenate([pair, first[0]])
    half_b = jnp.concatenate([first[2], first[1]])
    a1 = send(half_a, crosswise(1, False))
    a3 = send(half_a, crosswise(3, False))
    b3 = send(half_b, crosswise(3, False))
    b1 = send(half_b, crosswise(1, False))
    a2 = send(a3, crosswise(1, False))
    b2 = send(b1, crosswise(3, False))

    turned = context.T.reshape(4, quarter, tokens)
    block = jnp.stack(
        [at(turned, y)]
        + [send(at(turned, y ^ k), lambda x, h, y, l, c, k=k: (x, h, y ^ k, l, c)) for k in others]
    )
    mine = send(block, lambda x, h, y, l, c: (l, c, y, l ^ x, h))
    gathered = [mine] + [
        send(mine, lambda x, h, y, l, c, k=k: (x, h, y, l ^ k, c)) for k in (1, 2, 3)
    ]
    own = jnp.stack(gathered)
    swap = lambda x, h, y, l, c: (x, h, y, l, 1 - c)
    other = send(own, swap)

    corner = pl.pallas_call(
        touch_kernel,
        out_shape=jax.ShapeDtypeStruct((16, 128), BF16),
        in_specs=[VMEM],
        out_specs=VMEM,
        compiler_params=pltpu.CompilerParams(vmem_limit_bytes=12 * MIB),
        cost_estimate=pl.CostEstimate(flops=0, bytes_accessed=8192, transcendentals=0),
    )(out_weight)
    (given,) = products(out_weight, cotangent, far_cot, after=corner)
    taken = send(given, swap)
    at_home, after, before, skip_up, skip_down = products(out_weight, cotangent, far_cot, taken)
    from_before = send(after, ring(1))
    from_after = send(before, ring(-1))
    from_two_before = send(skip_up, ring(2))
    from_two_after = send(skip_down, ring(-2))

    early = [(k, 0, k, tokens, k, 0) for k in range(4)]
    halves = lambda a, k: [
        (a + n // 2, deep, a + n // 2, deep + tokens, i, k)
        for n, i in enumerate((0, 1, 3, 2))
        for deep in (n % 2 * 2 * tokens,)
    ]
    total = weight_part(early, own, other, [pair] + first)
    total = weight_part(halves(0, 1) + halves(2, 3), own, other, [a1, b1, a3, b3], total)
    grad_weight = weight_part(halves(0, 2), own, other, [a2, b2], total)
    grad_context = pl.pallas_call(
        finish_kernel,
        out_shape=jax.ShapeDtypeStruct((tokens, width), BF16),
        in_specs=[VMEM] * 5,
        out_specs=VMEM,
        compiler_params=pltpu.CompilerParams(vmem_limit_bytes=8 * MIB),
        cost_estimate=pl.CostEstimate(
            flops=4 * tokens * width, bytes_accessed=18 * tokens * width, transcendentals=0
        ),
    )(at_home, from_before, from_after, from_two_before, from_two_after)
    return grad_weight, grad_context


def solution(mesh):
    return jax.shard_map(
        step,
        mesh=mesh,
        in_specs=(P(("batch", "seq"), "mp"), P(("batch", "seq"), "mp"), P(None, "mp")),
        out_specs=(P(("batch", "seq"), "mp"), P(("batch", "seq"), "mp")),
        check_vma=False,
    )
```
